512 devices in a mesh: img: 2 (over y), row: 128 (over x, z), col: 2 (over core).
Axes of the slice: x: 4, y: 2, z: 32, core: 2. Of those that a mesh axis runs over, the one named last changes fastest.
The devices are a block of a 4x8x32 slice.
Arguments:
- features: bfloat16 [256, 128, 512], P(('img', 'row'), 'col'), parts along dimension 0, may hold values from -60 to 60
- first_gain: float32 [512], replicated, may hold values from 0.1 to 1.9
- first_shift: float32 [512], replicated, may hold values from -2.5 to 2.5
- first_weight: bfloat16 [3, 3, 512, 512], P(None, None, 'row'), may hold values from -0.09375 to 0.09375
- first_bias: float32 [512], replicated, may hold values from -2.5 to 2.5
- second_gain: float32 [512], replicated, may hold values from 0.1 to 1.9
- second_shift: float32 [512], replicated, may hold values from -2.5 to 2.5
- second_weight: bfloat16 [3, 3, 512, 512], P(None, None, 'row'), may hold values from -0.09375 to 0.09375
- second_bias: float32 [512], replicated, may hold values from -2.5 to 2.5
- upsample_weight: bfloat16 [3, 3, 512, 512], P(None, None, 'row'), may hold values from -0.09375 to 0.09375
- upsample_bias: float32 [512], replicated, may hold values from -2.5 to 2.5
Outputs:
- upsampled: bfloat16 [512, 256, 512], P(('img', 'row'), 'col'), parts along dimension 0
The draws below stay inside these ranges and needn't reach their ends.
There are 2 independent parts, one for each index of `img`. The reference program is written for one: setup_inputs(seed, part) draws one part's arguments, and reference() takes and returns one part's arrays. A program takes and returns all parts, laid end to end along the dimension named above; an argument that names none is the same for every part. Nothing has to cross between parts.
All inputs are finite; a program needn't handle non-finite values.
Results may differ from the reference program's by a relative error of at most 0.0075.
Values may be sent and summed in bfloat16 or wider, within the bound.
No kernel may reach another device: no remote copies, remote signals or barrier semaphores. Data moves between devices by JAX's collectives and lax.ppermute only.
A program may use at most 128 MiB of HBM per device.

```python
import math
import jax
import jax.numpy as jnp
from jax import lax

C = 512
G = 32
H = 128
W = 128


def draw_features(key, part):
    subkeys = jax.random.split(key, 4)
    heights = jnp.arange(H, dtype=jnp.float32) / max(H - 1, 1)
    trend = jnp.exp(heights * math.log(3.0))
    row_jitter = jnp.exp(jax.random.uniform(subkeys[1], (H,), jnp.float32, 0.0, math.log(1.6)))
    column_jitter = jnp.exp(jax.random.uniform(subkeys[2], (W,), jnp.float32, 0.0, math.log(1.6)))
    channel_scale = jnp.exp(jax.random.uniform(subkeys[3], (C,), jnp.float32, math.log(0.7), math.log(1.4)))
    base = jnp.clip(jax.random.normal(subkeys[0], (H, W, C), jnp.float32), -5.0, 5.0)
    scale = trend[:, None, None] * row_jitter[:, None, None] * column_jitter[None, :, None] * channel_scale[None, None, :]
    return (base * scale).astype(jnp.bfloat16)


def level_of(stream_key, shape, shards, smallest, high):
    def one(axis_at, shards_of):
        steps = jax.random.uniform(jax.random.fold_in(jax.random.fold_in(stream_key, 6), axis_at), (shards_of,), jnp.float32, smallest / len(shards), high / len(shards))
        return jnp.repeat(jnp.exp(steps), shape[axis_at] // shards_of).reshape((-1,) + (1,) * (len(shape) - axis_at - 1))

    loudness = one(*shards[0])
    for cut in shards[1:]:
        loudness = loudness * one(*cut)
    return loudness


def bell_draw(rng, extent, spread, reach, shards=(), held_as=jnp.bfloat16):
    values = jax.random.normal(rng, extent, jnp.float32) * spread
    if len(shards) > 0:
        values = level_of(rng, extent, shards, -0.22, 0.18) * values
    return jnp.clip(values, min=-reach, max=reach).astype(held_as)


def setup_inputs(seed: int = 0, part: int = 0) -> dict:
    streams_of = jax.random.split(jax.random.key(seed), 12)
    part_splits = jax.random.split(jax.random.fold_in(streams_of[11], part), 12)
    return {
        "features": draw_features(jax.random.fold_in(jax.random.fold_in(streams_of[11], part), 71), part),
        "first_gain": jnp.clip(1.0 + 0.18 * jax.random.normal(streams_of[1], (C,), jnp.float32), 0.1, 1.9),
        "first_shift": bell_draw(streams_of[2], (C,), 0.5, 2.5, (), jnp.float32),
        "first_weight": bell_draw(streams_of[3], (3, 3, C, C), (9 * C) ** -0.5, 0.09375, ((2, 128),)),
        "first_bias": bell_draw(streams_of[4], (C,), 0.5, 2.5, (), jnp.float32),
        "second_gain": jnp.clip(1.0 + 0.18 * jax.random.normal(streams_of[5], (C,), jnp.float32), 0.1, 1.9),
        "second_shift": bell_draw(streams_of[6], (C,), 0.5, 2.5, (), jnp.float32),
        "second_weight": bell_draw(streams_of[7], (3, 3, C, C), (9 * C) ** -0.5, 0.09375, ((2, 128),)),
        "second_bias": bell_draw(streams_of[8], (C,), 0.5, 2.5, (), jnp.float32),
        "upsample_weight": bell_draw(streams_of[9], (3, 3, C, C), (9 * C) ** -0.5, 0.09375, ((2, 128),)),
        "upsample_bias": bell_draw(streams_of[10], (C,), 0.5, 2.5, (), jnp.float32),
    }


EPS = 1e-06

def group_norm_silu(values, gain, shift):
    height, breadth, channels = values.shape
    grouped = values.reshape(height * breadth, G, channels // G)
    total = lax.optimization_barrier(jnp.sum(grouped, axis=(0, 2)))
    squares = lax.optimization_barrier(jnp.sum(grouped * grouped, axis=(0, 2)))
    count = height * breadth * (channels // G)
    mean = total / count
    var = squares / count - mean * mean
    factor = lax.rsqrt(var + EPS)
    normed = (grouped - mean[None, :, None]) * factor[None, :, None]
    normed = normed.reshape(height, breadth, channels) * gain + shift
    return jax.nn.silu(normed).astype(jnp.bfloat16)

def convolve(inputs, weight, bias):
    result = lax.conv_general_dilated(inputs.astype(jnp.float32)[None], weight.astype(jnp.float32), (1, 1), 'SAME', dimension_numbers=('NHWC', 'HWIO', 'NHWC'), precision=lax.Precision.HIGHEST)
    return result[0] + bias

def reference(features, first_gain, first_shift, first_weight, first_bias, second_gain, second_shift, second_weight, second_bias, upsample_weight, upsample_bias):
    normed_one = group_norm_silu(features.astype(jnp.float32), first_gain, first_shift)
    hidden = convolve(normed_one, first_weight, first_bias).astype(jnp.bfloat16)
    normed_two = group_norm_silu(hidden.astype(jnp.float32), second_gain, second_shift)
    block_out = (convolve(normed_two, second_weight, second_bias) + features.astype(jnp.float32)).astype(jnp.bfloat16)
    doubled = jnp.repeat(jnp.repeat(block_out, 2, axis=0), 2, axis=1)
    return convolve(doubled, upsample_weight, upsample_bias).astype(jnp.bfloat16)
```

```python
import functools

import jax
import jax.numpy as jnp
from jax import lax
from jax.experimental import pallas as pl
from jax.experimental.pallas import tpu as pltpu
from jax.sharding import Mesh
from jax.sharding import PartitionSpec as P

G = 32
EPS = 1e-06
F32, BF16 = jnp.float32, jnp.bfloat16
HIGHEST = lax.Precision.HIGHEST
ROW = ("x", "z")
IMG_ROW = ("img", "x", "z")


def sum_over(vector, axes):
    count = lax.axis_size(axes)
    sent = jnp.broadcast_to(vector, (count, vector.shape[1]))
    return lax.all_to_all(sent, axes, 0, 0, tiled=True)


def shifted_rows(values, axis, by):
    count = lax.axis_size(axis)
    pairs = [(i, i - by) for i in range(count) if 0 <= i - by < count]
    return lax.ppermute(values, axis, pairs)


def put_shifted(S, row, cols, y, lanes):
    at = pl.ds(row * cols, cols)
    column = lax.broadcasted_iota(jnp.int32, y.shape, 0)
    S[1, at, lanes] = y.astype(BF16)
    S[0, at, lanes] = jnp.where(column == 0, 0.0, pltpu.roll(y, 1, 0)).astype(BF16)
    S[2, at, lanes] = jnp.where(column == cols - 1, 0.0, pltpu.roll(y, cols - 1, 0)).astype(BF16)


def silu(u):
    return u / (1.0 + jnp.exp(-u))


def conv_one_kernel(cols, rows, image_rows, at_ref, x_ref, a_ref, b_ref, bias_ref, pick_ref, w_ref, out_ref, sums_ref, S, acc):
    t = pl.program_id(0)
    first = at_ref[0] - 3
    outs = acc.shape[1]

    @pl.when(t == 0)
    def _():
        for i in range(rows + 2):
            x = x_ref[pl.ds(i * cols, cols), :].astype(F32)
            y = silu(x * a_ref[...] + b_ref[...])
            inside = jnp.logical_and(first + i >= 0, first + i < image_rows)
            y = jnp.where(inside, y, 0.0)
            put_shifted(S, i, cols, y, slice(None))
        acc[...] = jnp.broadcast_to(bias_ref[...], acc.shape)

    start = pl.multiple_of((t // 3) * cols, cols)
    piece = w_ref[...].reshape(-1, outs)
    acc[...] += jnp.dot(S[t % 3, pl.ds(start, rows * cols), :], piece, preferred_element_type=F32)

    @pl.when(t == 8)
    def _():
        hidden = acc[...].astype(BF16)
        out_ref[...] = hidden
        mid = rows // 2
        own = hidden[mid * cols : (mid + 1) * cols].astype(F32)
        both = jnp.concatenate(
            [jnp.sum(own, axis=0, keepdims=True), jnp.sum(own * own, axis=0, keepdims=True)], axis=1
        )
        both = jnp.broadcast_to(both, (8, 2 * outs))
        sums_ref[...] = jnp.dot(both, pick_ref[...], precision=HIGHEST, preferred_element_type=F32)


def norm_kernel(cols, rows, image_rows, count, groups, at_ref, x_ref, stats_ref, gain_ref, shift_ref, pick_ref, out_ref):
    totals = jnp.sum(stats_ref[...], axis=0, keepdims=True)
    totals = jnp.broadcast_to(totals, (8, totals.shape[1]))
    spread = lax.dot_general(
        totals, pick_ref[...], (((1,), (1,)), ((), ())), precision=HIGHEST, preferred_element_type=F32
    )
    outs = gain_ref.shape[1]
    mean = spread[:1, :outs] / count
    var = spread[:1, outs:] / count - mean * mean
    a = lax.rsqrt(var + EPS) * gain_ref[...]
    b = shift_ref[...] - mean * a
    first = at_ref[0] - rows // 2
    for i in range(rows):
        at = pl.ds(i * cols, cols)
        y = silu(x_ref[at, :].astype(F32) * a + b)
        inside = jnp.logical_and(first + i >= 0, first + i < image_rows)
        out_ref[at, :] = jnp.where(inside, y, 0.0).astype(BF16)


def conv_two_kernel(cols, rows, image_rows, at_ref, x_ref, res_ref, bias_ref, w_ref, out_ref, S, acc):
    t = pl.program_id(0)
    outs = acc.shape[1]

    @pl.when(t == 0)
    def _():
        for i in range(rows + 2):
            for h in range(2):
                y = x_ref[h, pl.ds(i * cols, cols), :].astype(F32)
                put_shifted(S, i, cols, y, slice(h * outs, (h + 1) * outs))
        acc[...] = jnp.broadcast_to(bias_ref[...], acc.shape)

    start = pl.multiple_of((t // 3) * cols, cols)
    piece = w_ref[...].reshape(-1, outs)
    acc[...] += jnp.dot(S[t % 3, pl.ds(start, rows * cols), :], piece, preferred_element_type=F32)

    @pl.when(t == 8)
    def _():
        first = at_ref[0] - rows // 2
        for i in range(rows):
            at = pl.ds(i * cols, cols)
            y = acc[at, :] + res_ref[at, :].astype(F32)
            inside = jnp.logical_and(first + i >= 0, first + i < image_rows)
            out_ref[at, :] = jnp.where(inside, y, 0.0).astype(BF16)


def conv_up_kernel(cols, x_ref, bias_ref, w_ref, out_ref, S, acc, full):
    t = pl.program_id(0)
    outs = acc.shape[2]

    @pl.when(t == 0)
    def _():
        for i in range(3):
            for h in range(2):
                y = x_ref[h, pl.ds(i * cols, cols), :].astype(F32)
                put_shifted(S, i, cols, y, slice(h * outs, (h + 1) * outs))
        acc[...] = jnp.broadcast_to(bias_ref[...][None], acc.shape)

    a, c = t // 3, t % 3
    piece = w_ref[...].reshape(-1, outs)
    for p in range(2):
        for q in range(2):
            start = pl.multiple_of(((a + 1 + p) // 2) * cols, cols)
            acc[2 * p + q] += jnp.dot(
                S[(c + 1 + q) // 2, pl.ds(start, cols), :], piece, preferred_element_type=F32
            )

    @pl.when(t == 8)
    def _():
        for p in range(2):
            for q in range(2):
                for k in range(2):
                    lanes = slice(k * 128, (k + 1) * 128)
                    full[p, k, pl.ds(q, cols, stride=2), :] = acc[2 * p + q][:, lanes]
            for k in range(2):
                for half in range(2):
                    out_ref[half, p, :, k * 128 : (k + 1) * 128] = full[
                        p, k, half * cols : (half + 1) * cols, :
                    ].astype(BF16)


VM = pl.BlockSpec(memory_space=pltpu.VMEM)
SM = pl.BlockSpec(memory_space=pltpu.SMEM)


def weight_spec(gathered, base):
    n, _, rows, outs = gathered.shape
    return pl.BlockSpec((n, 1, rows, outs), lambda t: (0, base + t, 0, 0))


def on_device(
    features,
    first_gain,
    first_shift,
    first_weight,
    first_bias,
    second_gain,
    second_shift,
    second_weight,
    second_bias,
    upsample_weight,
    upsample_bias,
):
    _, breadth, channels = features.shape
    nx, nz, ncol = lax.axis_size("x"), lax.axis_size("z"), lax.axis_size("col")
    k_own = first_weight.shape[2]
    cols = breadth * ncol
    half = channels // ncol
    image_rows = nx * nz
    per_group = channels // G
    count = image_rows * cols * per_group
    c = lax.axis_index("col")
    at = (lax.axis_index("x") * nz + lax.axis_index("z")).astype(jnp.int32)[None]

    def reorder(v):
        return v.reshape(-1, nx, nz, k_own).transpose(0, 2, 1, 3).reshape(-1, channels)

    natural = lax.broadcasted_iota(jnp.int32, (channels, channels), 0)
    place = lax.broadcasted_iota(jnp.int32, (channels, channels), 1)
    source = (place // k_own) % nx * (nz * k_own) + place // (k_own * nx) * k_own + place % k_own
    move = (natural == source).astype(BF16)

    def moved(v):
        return jnp.dot(v, move, preferred_element_type=F32).astype(BF16)

    def own_half(v):
        return lax.dynamic_slice_in_dim(v, c * half, half, v.ndim - 1)

    taps = 9 * k_own
    hold = moved(
        jnp.concatenate([first_weight.reshape(taps, channels), second_weight.reshape(taps, channels)])
    )
    hold = jnp.concatenate([hold, upsample_weight.reshape(taps, channels)])
    hold = own_half(hold).reshape(1, 27, k_own, half)
    hold = lax.all_to_all(jnp.broadcast_to(hold, (nx, 27, k_own, half)), "x", 0, 0, tiled=True)
    hold = hold.transpose(1, 0, 2, 3).reshape(27, nx * k_own, half)
    weights = lax.all_gather(hold, "z")

    own = features[0]
    own_moved = moved(own)
    ext = jnp.stack(
        [shifted_rows(own_moved, ROW, d) if d else own_moved for d in range(-3, 4)]
    )
    ext = lax.all_gather(ext, "col", axis=1, tiled=True).reshape(7 * cols, channels)

    wide = own.astype(F32)
    chan = lax.broadcasted_iota(jnp.int32, (channels, G), 0) // per_group
    member = (chan == lax.broadcasted_iota(jnp.int32, (channels, G), 1)).astype(F32)
    sums = jnp.stack([jnp.sum(wide, axis=0), jnp.sum(wide * wide, axis=0)])
    sums = jnp.dot(sums, member, precision=HIGHEST).reshape(1, 2 * G)
    sums = jnp.pad(sums, ((0, 0), (0, 128 - 2 * G)))
    sums = jnp.sum(sum_over(sums, ("x", "col")), axis=0, keepdims=True)
    sums = jnp.sum(sum_over(sums, "z"), axis=0)
    mean = sums[:G] / count
    var = sums[G : 2 * G] / count - mean * mean
    factor = lax.rsqrt(var + EPS)
    both = jnp.repeat(jnp.stack([mean, factor]), per_group, axis=1)
    a = both[1] * first_gain
    b = first_shift - both[0] * a
    ab = reorder(jnp.stack([a, b]))

    vectors = reorder(jnp.stack([first_bias, second_gain, second_shift, second_bias]))
    vectors = own_half(jnp.concatenate([vectors, upsample_bias[None]]))
    bias_one, gain_two, shift_two, bias_two, bias_up = [vectors[i : i + 1] for i in range(5)]

    groups = G // ncol
    lane = jnp.arange(half)
    group = lane // (per_group // k_own * nx * k_own) * nx + lane // k_own % nx
    pick = group[:, None] == jnp.arange(128)[None, :]
    pick = jnp.concatenate([pick, jnp.roll(pick, groups, axis=1)]).astype(F32)

    rows = 5
    hidden, sums_two = pl.pallas_call(
        functools.partial(conv_one_kernel, cols, rows, image_rows),
        grid=(9,),
        out_shape=(
            jax.ShapeDtypeStruct((rows * cols, half), BF16),
            jax.ShapeDtypeStruct((8, 128), F32),
        ),
        in_specs=[SM, VM, VM, VM, VM, VM, weight_spec(weights, 0)],
        out_specs=(VM, VM),
        scratch_shapes=[
            pltpu.VMEM((3, (rows + 2) * cols, channels), BF16),
            pltpu.VMEM((rows * cols, half), F32),
        ],
        name="conv_one",
    )(at, ext, ab[:1], ab[1:], bias_one, pick, weights)

    stats = sum_over(sums_two[:1], ROW)
    normed = pl.pallas_call(
        functools.partial(norm_kernel, cols, rows, image_rows, count, groups),
        out_shape=jax.ShapeDtypeStruct((rows * cols, half), BF16),
        in_specs=[SM, VM, VM, VM, VM, VM],
        out_specs=VM,
        name="norm_two",
    )(at, hidden, stats, gain_two, shift_two, pick)
    normed = lax.all_gather(normed, "col")

    rows = 3
    residual = own_half(ext[2 * cols : 5 * cols])
    block = pl.pallas_call(
        functools.partial(conv_two_kernel, cols, rows, image_rows),
        grid=(9,),
        out_shape=jax.ShapeDtypeStruct((rows * cols, half), BF16),
        in_specs=[SM, VM, VM, VM, weight_spec(weights, 9)],
        out_specs=VM,
        scratch_shapes=[
            pltpu.VMEM((3, (rows + 2) * cols, channels), BF16),
            pltpu.VMEM((rows * cols, half), F32),
        ],
        name="conv_two",
    )(at, normed, residual, bias_two, weights)
    block = lax.all_gather(block, "col")

    up = pl.pallas_call(
        functools.partial(conv_up_kernel, cols),
        grid=(9,),
        out_shape=jax.ShapeDtypeStruct((ncol, 2, cols, half), BF16),
        in_specs=[VM, VM, weight_spec(weights, 18)],
        out_specs=VM,
        scratch_shapes=[
            pltpu.VMEM((3, 3 * cols, channels), BF16),
            pltpu.VMEM((4, cols, half), F32),
            pltpu.VMEM((2, 2, 2 * cols, 128), F32),
        ],
        name="conv_up",
    )(block, bias_up, weights)
    up = lax.all_to_all(up, "col", 0, 0, tiled=True)
    return up.transpose(1, 2, 0, 3).reshape(2, cols, channels)


def solution(mesh):
    finer = Mesh(
        mesh.devices.reshape(mesh.shape["img"], 4, 32, mesh.shape["col"]),
        ("img", "x", "z", "col"),
    )
    in_specs = (
        P(IMG_ROW, "col", None),
        P(),
        P(),
        P(None, None, ROW, None),
        P(),
        P(),
        P(),
        P(None, None, ROW, None),
        P(),
        P(None, None, ROW, None),
        P(),
    )
    return jax.shard_map(
        on_device,
        mesh=finer,
        in_specs=in_specs,
        out_specs=P(IMG_ROW, "col", None),
        check_vma=False,
    )
```

```python
import functools

import jax
import jax.numpy as jnp
from jax import lax
from jax.experimental import pallas as pl
from jax.experimental.pallas import tpu as pltpu
from jax.sharding import Mesh
from jax.sharding import PartitionSpec as P

G = 32
EPS = 1e-06
F32, BF16 = jnp.float32, jnp.bfloat16
HIGHEST = lax.Precision.HIGHEST
ROW = ("x", "zh", "zl")
IMG_ROW = ("img",) + ROW


def sum_over(vector, axes):
    count = lax.axis_size(axes)
    sent = jnp.broadcast_to(vector, (count, vector.shape[1]))
    return lax.all_to_all(sent, axes, 0, 0, tiled=True)


def shifted_rows(values, axis, by):
    count = lax.axis_size(axis)
    pairs = [(i, i - by) for i in range(count) if 0 <= i - by < count]
    return lax.ppermute(values, axis, pairs)


def put_shifted(S, row, cols, y, lanes):
    at = pl.ds(row * cols, cols)
    column = lax.broadcasted_iota(jnp.int32, y.shape, 0)
    S[1, at, lanes] = y.astype(BF16)
    S[0, at, lanes] = jnp.where(column == 0, 0.0, pltpu.roll(y, 1, 0)).astype(BF16)
    S[2, at, lanes] = jnp.where(column == cols - 1, 0.0, pltpu.roll(y, cols - 1, 0)).astype(BF16)


def silu(u):
    return u / (1.0 + jnp.exp(-u))


def spread_stats(stats, pick, count, gain, shift):
    totals = jnp.sum(stats, axis=0, keepdims=True)
    totals = jnp.broadcast_to(totals, (8, totals.shape[1]))
    spread = lax.dot_general(
        totals, pick, (((1,), (1,)), ((), ())), precision=HIGHEST, preferred_element_type=F32
    )
    width = gain.shape[1]
    mean = spread[:1, :width] / count
    var = spread[:1, width:] / count - mean * mean
    a = lax.rsqrt(var + EPS) * gain
    return a, shift - mean * a


def conv_one_kernel(cols, image_rows, count, at_ref, x_ref, stats_ref, gain_ref, shift_ref, pick_ref, w_ref, out_ref, S):
    quad, depth = x_ref.shape[0], x_ref.shape[3]
    a, b = spread_stats(stats_ref[...], pick_ref[...], count, gain_ref[...], shift_ref[...])
    first = at_ref[0] // quad * quad - 1
    column = lax.broadcasted_iota(jnp.int32, (cols, depth), 0)
    for i in range(quad + 2):
        member = min(max(i - 1, 0), quad - 1)
        slot = 0 if 1 <= i <= quad else 1
        y = silu(x_ref[member, slot].astype(F32) * a + b)
        if slot:
            y = jnp.where(jnp.logical_and(first + i >= 0, first + i < image_rows), y, 0.0)
        at = slice(i * cols, (i + 1) * cols)
        left = jnp.where(column == 0, 0.0, pltpu.roll(y, 1, 0))
        right = jnp.where(column == cols - 1, 0.0, pltpu.roll(y, cols - 1, 0))
        S[at, 0 * depth : 1 * depth] = left.astype(BF16)
        S[at, 1 * depth : 2 * depth] = y.astype(BF16)
        S[at, 2 * depth : 3 * depth] = right.astype(BF16)
    outs = out_ref.shape[2]
    total = jnp.zeros((quad * cols, outs), F32)
    for r in range(3):
        piece = jnp.concatenate([w_ref[:, 3 * r + k].reshape(depth, outs) for k in range(3)], axis=0)
        total += jnp.dot(S[r * cols : (r + quad) * cols, :], piece, preferred_element_type=F32)
    out_ref[...] = total.reshape(quad, cols, outs)


def join_kernel(x_ref, bias_ref, pick_ref, out_ref, sums_ref):
    total = x_ref[0]
    for k in range(1, x_ref.shape[0]):
        total += x_ref[k]
    hidden = (total + bias_ref[...]).astype(BF16)
    out_ref[...] = hidden
    own = hidden.astype(F32)
    both = jnp.concatenate(
        [jnp.sum(own, axis=0, keepdims=True), jnp.sum(own * own, axis=0, keepdims=True)], axis=1
    )
    both = jnp.broadcast_to(both, (8, both.shape[1]))
    sums_ref[...] = jnp.dot(both, pick_ref[...], precision=HIGHEST, preferred_element_type=F32)


def norm_kernel(rows, image_rows, count, at_ref, *refs):
    stats_ref, gain_ref, shift_ref, pick_ref, out_ref = refs[rows:]
    a, b = spread_stats(stats_ref[...], pick_ref[...], count, gain_ref[...], shift_ref[...])
    first = at_ref[0] - rows // 2
    for i in range(rows):
        y = silu(refs[i][...].astype(F32) * a + b)
        inside = jnp.logical_and(first + i >= 0, first + i < image_rows)
        cols = y.shape[0]
        out_ref[i * cols : (i + 1) * cols, :] = jnp.where(inside, y, 0.0).astype(BF16)


def conv_two_kernel(cols, rows, image_rows, at_ref, x_ref, res_ref, bias_ref, w_ref, out_ref, S, acc):
    t = pl.program_id(0)
    outs = acc.shape[1]

    @pl.when(t == 0)
    def _():
        for i in range(rows + 2):
            for h in range(2):
                y = x_ref[h, pl.ds(i * cols, cols), :].astype(F32)
                put_shifted(S, i, cols, y, slice(h * outs, (h + 1) * outs))
        acc[...] = jnp.broadcast_to(bias_ref[...], acc.shape)

    start = pl.multiple_of((t // 3) * cols, cols)
    piece = w_ref[...].reshape(-1, outs)
    acc[...] += jnp.dot(S[t % 3, pl.ds(start, rows * cols), :], piece, preferred_element_type=F32)

    @pl.when(t == 8)
    def _():
        first = at_ref[0] - rows // 2
        for i in range(rows):
            at = pl.ds(i * cols, cols)
            y = acc[at, :] + res_ref[at, :].astype(F32)
            inside = jnp.logical_and(first + i >= 0, first + i < image_rows)
            out_ref[at, :] = jnp.where(inside, y, 0.0).astype(BF16)


def conv_up_kernel(cols, x_ref, bias_ref, w_ref, out_ref, S, acc, full):
    t = pl.program_id(0)
    outs = acc.shape[2]

    @pl.when(t == 0)
    def _():
        for i in range(3):
            for h in range(2):
                y = x_ref[h, pl.ds(i * cols, cols), :].astype(F32)
                put_shifted(S, i, cols, y, slice(h * outs, (h + 1) * outs))
        acc[...] = jnp.broadcast_to(bias_ref[...][None], acc.shape)

    a, c = t // 3, t % 3
    piece = w_ref[...].reshape(-1, outs)
    for p in range(2):
        for q in range(2):
            start = pl.multiple_of(((a + 1 + p) // 2) * cols, cols)
            acc[2 * p + q] += jnp.dot(
                S[(c + 1 + q) // 2, pl.ds(start, cols), :], piece, preferred_element_type=F32
            )

    @pl.when(t == 8)
    def _():
        for p in range(2):
            for q in range(2):
                for k in range(2):
                    lanes = slice(k * 128, (k + 1) * 128)
                    full[p, k, pl.ds(q, cols, stride=2), :] = acc[2 * p + q][:, lanes]
            for k in range(2):
                for half in range(2):
                    out_ref[half, p, :, k * 128 : (k + 1) * 128] = full[
                        p, k, half * cols : (half + 1) * cols, :
                    ].astype(BF16)


VM = pl.BlockSpec(memory_space=pltpu.VMEM)
SM = pl.BlockSpec(memory_space=pltpu.SMEM)


def weight_spec(gathered, base):
    n, _, rows, outs = gathered.shape
    return pl.BlockSpec((n, 1, rows, outs), lambda t: (0, base + t, 0, 0))


def on_device(
    features,
    first_gain,
    first_shift,
    first_weight,
    first_bias,
    second_gain,
    second_shift,
    second_weight,
    second_bias,
    upsample_weight,
    upsample_bias,
):
    _, breadth, channels = features.shape
    nx, nzh, nzl, ncol = (lax.axis_size(axis) for axis in ("x", "zh", "zl", "col"))
    nz = nzh * nzl
    k_own = first_weight.shape[2]
    cols = breadth * ncol
    half = channels // ncol
    depth = channels // nzl
    image_rows = nx * nz
    per_group = channels // G
    count = image_rows * cols * per_group
    c = lax.axis_index("col")
    zl = lax.axis_index("zl")
    at = lax.axis_index(ROW).astype(jnp.int32)[None]

    def order(v, axes):
        v = v.reshape(-1, nx, nzh, nzl, k_own).transpose(0, *[k + 1 for k in axes], 4)
        return v.reshape(-1, channels)

    place = lax.broadcasted_iota(jnp.int32, (channels, channels), 1)
    natural = lax.broadcasted_iota(jnp.int32, (channels, channels), 0)
    k, x = place % k_own, place // k_own % nx
    line = place // (k_own * nx)
    source = (x * nz + line) * k_own + k
    move = (natural == source).astype(BF16)
    source = (x * nz + line % nzh * nzl + line // nzh) * k_own + k
    move_one = (natural == source).astype(BF16)

    def moved(v, by):
        return jnp.dot(v, by, preferred_element_type=F32).astype(BF16)

    def own_half(v):
        return lax.dynamic_slice_in_dim(v, c * half, half, v.ndim - 1)

    taps = 9 * k_own
    hold = moved(
        jnp.concatenate([first_weight.reshape(taps, channels), second_weight.reshape(taps, channels)]),
        move,
    )
    hold = jnp.concatenate([hold, upsample_weight.reshape(taps, channels)])
    hold = own_half(hold).reshape(1, 27, k_own, half)
    hold = lax.all_to_all(jnp.broadcast_to(hold, (nx, 27, k_own, half)), "x", 0, 0, tiled=True)
    hold = hold.transpose(1, 0, 2, 3).reshape(27, nx * k_own, half)
    weights = lax.all_gather(hold[9:], ("zh", "zl"))
    weights_one = lax.all_gather(hold[:9], "zh")

    own = features[0]
    wide = own.astype(F32)
    chan = lax.broadcasted_iota(jnp.int32, (channels, G), 0) // per_group
    member = (chan == lax.broadcasted_iota(jnp.int32, (channels, G), 1)).astype(F32)
    sums = jnp.stack([jnp.sum(wide, axis=0), jnp.sum(wide * wide, axis=0)])
    sums = jnp.dot(sums, member, precision=HIGHEST).reshape(1, 2 * G)
    sums = jnp.pad(sums, ((0, 0), (0, 128 - 2 * G)))
    sums = jnp.sum(sum_over(sums, ("x", "col")), axis=0, keepdims=True)
    sums = sum_over(sums, ("zh", "zl"))

    up_row, down_row = shifted_rows(own, ROW, -1), shifted_rows(own, ROW, 1)
    three = lax.all_gather(jnp.stack([up_row, own, down_row]), "col", axis=1, tiled=True)
    residual = own_half(moved(three.reshape(3 * cols, channels), move))
    edge = jnp.where(zl == 0, three[0], three[2])
    sent = moved(jnp.concatenate([three[1], edge]), move_one)
    sent = sent.reshape(2, cols, nzl, depth).transpose(2, 0, 1, 3)
    quad = lax.all_to_all(sent, "zl", 0, 0, tiled=True)

    def own_depth(v):
        return lax.dynamic_slice_in_dim(v, zl * depth, depth, 1)

    gain_one = own_depth(order(first_gain, (2, 1, 0)))
    shift_one = own_depth(order(first_shift, (2, 1, 0)))
    vectors = order(jnp.stack([first_bias, second_gain, second_shift, second_bias]), (1, 2, 0))
    vectors = own_half(jnp.concatenate([vectors, upsample_bias[None]]))
    bias_one, gain_two, shift_two, bias_two, bias_up = [vectors[i : i + 1] for i in range(5)]

    def picks(group, groups):
        pick = group[:, None] == jnp.arange(128)[None, :]
        return jnp.concatenate([pick, jnp.roll(pick, groups, axis=1)]).astype(F32)

    lane = jnp.arange(depth)
    pick_one = picks(lane // k_own % nx * nzh + lane // (k_own * nx), G)
    lane = jnp.arange(half)
    pick = picks(lane // (k_own * nx * nzl) * nx + lane // k_own % nx, G // ncol)

    parts = pl.pallas_call(
        functools.partial(conv_one_kernel, cols, image_rows, count),
        out_shape=jax.ShapeDtypeStruct((nzl, cols, half), F32),
        in_specs=[SM] + [VM] * 6,
        out_specs=VM,
        scratch_shapes=[pltpu.VMEM(((nzl + 2) * cols, 3 * depth), BF16)],
        name="conv_one",
    )(at, quad, sums, gain_one, shift_one, pick_one, weights_one)
    parts = lax.all_to_all(parts, "zl", 0, 0, tiled=True)
    hidden, sums_two = pl.pallas_call(
        join_kernel,
        out_shape=(
            jax.ShapeDtypeStruct((cols, half), BF16),
            jax.ShapeDtypeStruct((8, 128), F32),
        ),
        in_specs=[VM] * 3,
        out_specs=(VM, VM),
        name="join_one",
    )(parts, bias_one, pick)

    stats = jnp.sum(sum_over(sums_two[:1], ("x", "zl")), axis=0, keepdims=True)
    stats = sum_over(stats, "zh")
    five = [hidden if d == 0 else shifted_rows(hidden, ROW, d) for d in range(-2, 3)]
    normed = pl.pallas_call(
        functools.partial(norm_kernel, 5, image_rows, count),
        out_shape=jax.ShapeDtypeStruct((5 * cols, half), BF16),
        in_specs=[SM] + [VM] * 9,
        out_specs=VM,
        name="norm_two",
    )(at, *five, stats, gain_two, shift_two, pick)
    normed = lax.all_gather(normed, "col")

    rows = 3
    block = pl.pallas_call(
        functools.partial(conv_two_kernel, cols, rows, image_rows),
        grid=(9,),
        out_shape=jax.ShapeDtypeStruct((rows * cols, half), BF16),
        in_specs=[SM, VM, VM, VM, weight_spec(weights, 0)],
        out_specs=VM,
        scratch_shapes=[
            pltpu.VMEM((3, (rows + 2) * cols, channels), BF16),
            pltpu.VMEM((rows * cols, half), F32),
        ],
        name="conv_two",
    )(at, normed, residual, bias_two, weights)
    block = lax.all_gather(block, "col")

    up = pl.pallas_call(
        functools.partial(conv_up_kernel, cols),
        grid=(9,),
        out_shape=jax.ShapeDtypeStruct((ncol, 2, cols, half), BF16),
        in_specs=[VM, VM, weight_spec(weights, 9)],
        out_specs=VM,
        scratch_shapes=[
            pltpu.VMEM((3, 3 * cols, channels), BF16),
            pltpu.VMEM((4, cols, half), F32),
            pltpu.VMEM((2, 2, 2 * cols, 128), F32),
        ],
        name="conv_up",
    )(block, bias_up, weights)
    up = lax.all_to_all(up, "col", 0, 0, tiled=True)
    return up.transpose(1, 2, 0, 3).reshape(2, cols, channels)


def solution(mesh):
    finer = Mesh(
        mesh.devices.reshape(mesh.shape["img"], 4, 8, 4, mesh.shape["col"]),
        IMG_ROW + ("col",),
    )
    in_specs = (
        P(IMG_ROW, "col", None),
        P(),
        P(),
        P(None, None, ROW, None),
        P(),
        P(),
        P(),
        P(None, None, ROW, None),
        P(),
        P(None, None, ROW, None),
        P(),
    )
    return jax.shard_map(
        on_device,
        mesh=finer,
        in_specs=in_specs,
        out_specs=P(IMG_ROW, "col", None),
        check_vma=False,
    )
```

```python
import functools

import jax
import jax.numpy as jnp
from jax import lax
from jax.experimental import pallas as pl
from jax.experimental.pallas import tpu as pltpu
from jax.sharding import Mesh
from jax.sharding import PartitionSpec as P

G = 32
EPS = 1e-06
F32, BF16 = jnp.float32, jnp.bfloat16
HIGHEST = lax.Precision.HIGHEST
ROW = ("x", "zh", "zl")
IMG_ROW = ("img",) + ROW


def sum_over(vector, axes):
    count = lax.axis_size(axes)
    sent = jnp.broadcast_to(vector, (count, vector.shape[1]))
    return lax.all_to_all(sent, axes, 0, 0, tiled=True)


def shifted_rows(values, axis, by):
    count = lax.axis_size(axis)
    pairs = [(i, i - by) for i in range(count) if 0 <= i - by < count]
    return lax.ppermute(values, axis, pairs)


def put_shifted(S, row, cols, y, lanes):
    at = pl.ds(row * cols, cols)
    column = lax.broadcasted_iota(jnp.int32, y.shape, 0)
    S[1, at, lanes] = y.astype(BF16)
    S[0, at, lanes] = jnp.where(column == 0, 0.0, pltpu.roll(y, 1, 0)).astype(BF16)
    S[2, at, lanes] = jnp.where(column == cols - 1, 0.0, pltpu.roll(y, cols - 1, 0)).astype(BF16)


def silu(u):
    return u / (1.0 + jnp.exp(-u))


def spread_stats(stats, pick, count, gain, shift):
    totals = jnp.sum(stats, axis=0, keepdims=True)
    totals = jnp.broadcast_to(totals, (8, totals.shape[1]))
    spread = lax.dot_general(
        totals, pick, (((1,), (1,)), ((), ())), precision=HIGHEST, preferred_element_type=F32
    )
    width = gain.shape[1]
    mean = spread[:1, :width] / count
    var = spread[:1, width:] / count - mean * mean
    a = lax.rsqrt(var + EPS) * gain
    return a, shift - mean * a


def conv_one_kernel(cols, image_rows, count, at_ref, x_ref, stats_ref, gain_ref, shift_ref, pick_ref, w_ref, out_ref, S):
    quad, depth = x_ref.shape[0], x_ref.shape[4]
    a, b = spread_stats(stats_ref[...], pick_ref[...], count, gain_ref[...], shift_ref[...])
    first = at_ref[0] // quad * quad - 1
    column = lax.broadcasted_iota(jnp.int32, (cols, depth), 0)
    for i in range(quad + 2):
        member = min(max(i - 1, 0), quad - 1)
        slot = 0 if 1 <= i <= quad else 1
        x = jnp.concatenate([x_ref[member, h, slot] for h in range(x_ref.shape[1])], axis=0)
        y = silu(x.astype(F32) * a + b)
        if slot:
            y = jnp.where(jnp.logical_and(first + i >= 0, first + i < image_rows), y, 0.0)
        at = slice(i * cols, (i + 1) * cols)
        left = jnp.where(column == 0, 0.0, pltpu.roll(y, 1, 0))
        right = jnp.where(column == cols - 1, 0.0, pltpu.roll(y, cols - 1, 0))
        S[at, 0 * depth : 1 * depth] = left.astype(BF16)
        S[at, 1 * depth : 2 * depth] = y.astype(BF16)
        S[at, 2 * depth : 3 * depth] = right.astype(BF16)
    outs = out_ref.shape[2]
    total = jnp.zeros((quad * cols, outs), F32)
    for r in range(3):
        piece = jnp.concatenate([w_ref[:, 3 * r + k].reshape(depth, outs) for k in range(3)], axis=0)
        total += jnp.dot(S[r * cols : (r + quad) * cols, :], piece, preferred_element_type=F32)
    out_ref[...] = total.astype(BF16).reshape(quad, cols, outs)


def join_kernel(x_ref, bias_ref, pick_ref, out_ref, sums_ref):
    total = x_ref[0].astype(F32)
    for k in range(1, x_ref.shape[0]):
        total += x_ref[k].astype(F32)
    hidden = (total + bias_ref[...]).astype(BF16)
    out_ref[...] = hidden
    own = hidden.astype(F32)
    both = jnp.concatenate(
        [jnp.sum(own, axis=0, keepdims=True), jnp.sum(own * own, axis=0, keepdims=True)], axis=1
    )
    both = jnp.broadcast_to(both, (8, both.shape[1]))
    sums_ref[...] = jnp.dot(both, pick_ref[...], precision=HIGHEST, preferred_element_type=F32)


def norm_kernel(image_rows, count, at_ref, x_ref, stats_ref, gain_ref, shift_ref, pick_ref, out_ref):
    a, b = spread_stats(stats_ref[...], pick_ref[...], count, gain_ref[...], shift_ref[...])
    halves, rows, cols, half = x_ref.shape
    first = at_ref[0] - rows // 2
    for i in range(rows):
        inside = jnp.logical_and(first + i >= 0, first + i < image_rows)
        for h in range(halves):
            lanes = slice(h * half, (h + 1) * half)
            y = silu(x_ref[h, i].astype(F32) * a[:, lanes] + b[:, lanes])
            out_ref[h, i * cols : (i + 1) * cols, :] = jnp.where(inside, y, 0.0).astype(BF16)


def conv_two_kernel(cols, rows, image_rows, at_ref, x_ref, res_ref, bias_ref, w_ref, out_ref, S, acc):
    t = pl.program_id(0)
    outs = acc.shape[1]

    @pl.when(t == 0)
    def _():
        for i in range(rows + 2):
            for h in range(2):
                y = x_ref[h, pl.ds(i * cols, cols), :].astype(F32)
                put_shifted(S, i, cols, y, slice(h * outs, (h + 1) * outs))
        acc[...] = jnp.broadcast_to(bias_ref[...], acc.shape)

    start = pl.multiple_of(t * cols, cols)
    total = acc[...]
    for k in range(3):
        piece = w_ref[:, k].reshape(-1, outs)
        total += jnp.dot(S[k, pl.ds(start, rows * cols), :], piece, preferred_element_type=F32)
    acc[...] = total

    @pl.when(t == 2)
    def _():
        first = at_ref[0] - rows // 2
        for i in range(rows):
            at = pl.ds(i * cols, cols)
            y = acc[at, :] + res_ref[at, :].astype(F32)
            inside = jnp.logical_and(first + i >= 0, first + i < image_rows)
            out_ref[at, :] = jnp.where(inside, y, 0.0).astype(BF16)


def conv_up_kernel(cols, x_ref, bias_ref, w_ref, out_ref, S, acc, full):
    t = pl.program_id(0)
    outs = acc.shape[2]

    @pl.when(t == 0)
    def _():
        for i in range(3):
            for h in range(2):
                y = x_ref[h, pl.ds(i * cols, cols), :].astype(F32)
                put_shifted(S, i, cols, y, slice(h * outs, (h + 1) * outs))
        acc[...] = jnp.broadcast_to(bias_ref[...][None], acc.shape)

    for p in range(2):
        start = pl.multiple_of(((t + 1 + p) // 2) * cols, cols)
        for q in range(2):
            total = acc[2 * p + q]
            for k in range(3):
                total += jnp.dot(
                    S[(k + 1 + q) // 2, pl.ds(start, cols), :],
                    w_ref[:, k].reshape(-1, outs),
                    preferred_element_type=F32,
                )
            acc[2 * p + q] = total

    @pl.when(t == 2)
    def _():
        for p in range(2):
            for q in range(2):
                for k in range(2):
                    lanes = slice(k * 128, (k + 1) * 128)
                    full[p, k, pl.ds(q, cols, stride=2), :] = acc[2 * p + q][:, lanes]
            for k in range(2):
                for half in range(2):
                    out_ref[half, p, :, k * 128 : (k + 1) * 128] = full[
                        p, k, half * cols : (half + 1) * cols, :
                    ].astype(BF16)


VM = pl.BlockSpec(memory_space=pltpu.VMEM)
SM = pl.BlockSpec(memory_space=pltpu.SMEM)


def weight_spec(gathered, base):
    n, _, rows, outs = gathered.shape
    return pl.BlockSpec((n, 3, rows, outs), lambda t: (0, base + t, 0, 0))


def on_device(
    features,
    first_gain,
    first_shift,
    first_weight,
    first_bias,
    second_gain,
    second_shift,
    second_weight,
    second_bias,
    upsample_weight,
    upsample_bias,
):
    _, breadth, channels = features.shape
    nx, nzh, nzl, ncol = (lax.axis_size(axis) for axis in ("x", "zh", "zl", "col"))
    nz = nzh * nzl
    k_own = first_weight.shape[2]
    cols = breadth * ncol
    half = channels // ncol
    depth = channels // nzl
    image_rows = nx * nz
    per_group = channels // G
    count = image_rows * cols * per_group
    c = lax.axis_index("col")
    zl = lax.axis_index("zl")
    at = lax.axis_index(ROW).astype(jnp.int32)[None]

    def order(v, axes):
        v = v.reshape(-1, nx, nzh, nzl, k_own).transpose(0, *[k + 1 for k in axes], 4)
        return v.reshape(-1, channels)

    place = lax.broadcasted_iota(jnp.int32, (channels, channels), 1)
    natural = lax.broadcasted_iota(jnp.int32, (channels, channels), 0)
    k, x = place % k_own, place // k_own % nx
    line = place // (k_own * nx)
    source = (x * nz + line) * k_own + k
    move = (natural == source).astype(BF16)
    source = (x * nz + line % nzh * nzl + line // nzh) * k_own + k
    move_one = (natural == source).astype(BF16)

    def moved(v, by):
        return jnp.dot(v, by, preferred_element_type=F32).astype(BF16)

    def own_half(v):
        return lax.dynamic_slice_in_dim(v, c * half, half, v.ndim - 1)

    taps = 9 * k_own
    hold = moved(
        jnp.concatenate([first_weight.reshape(taps, channels), second_weight.reshape(taps, channels)]),
        move,
    )
    hold = jnp.concatenate([hold, upsample_weight.reshape(taps, channels)])
    hold = own_half(hold).reshape(1, 27, k_own, half)
    hold = lax.all_to_all(jnp.broadcast_to(hold, (nx, 27, k_own, half)), "x", 0, 0, tiled=True)
    hold = hold.transpose(1, 0, 2, 3).reshape(27, nx * k_own, half)
    weights = lax.all_gather(hold[9:], ("zh", "zl"))
    hold_one = hold[:9]

    own = features[0]
    wide = own.astype(F32)
    chan = lax.broadcasted_iota(jnp.int32, (channels, G), 0) // per_group
    member = (chan == lax.broadcasted_iota(jnp.int32, (channels, G), 1)).astype(F32)
    sums = jnp.stack([jnp.sum(wide, axis=0), jnp.sum(wide * wide, axis=0)])
    sums = jnp.dot(sums, member, precision=HIGHEST).reshape(1, 2 * G)
    sums = jnp.pad(sums, ((0, 0), (0, 128 - 2 * G)))
    sums = jnp.sum(sum_over(sums, ("x", "col")), axis=0, keepdims=True)

    up_row, down_row = shifted_rows(own, ROW, -1), shifted_rows(own, ROW, 1)
    edge = jnp.where(zl == 0, up_row, down_row)
    sent = moved(jnp.concatenate([own, edge]), move_one)
    sent = sent.reshape(2, breadth, nzl, depth).transpose(2, 0, 1, 3)
    sent = jnp.broadcast_to(sent[:, None], (nzl, ncol, 2, breadth, depth))
    sent = sent.reshape(nzl * ncol, 2, breadth, depth)
    quad = lax.all_to_all(sent, ("zl", "col"), 0, 0, tiled=True)

    sums, hold_one, quad = lax.optimization_barrier((sums, hold_one, quad))
    sums = sum_over(sums, ("zh", "zl"))
    weights_one = lax.all_gather(hold_one, "zh")
    quad = quad.reshape(nzl, ncol, 2, breadth, depth)

    def own_depth(v):
        return lax.dynamic_slice_in_dim(v, zl * depth, depth, 1)

    gain_one = own_depth(order(first_gain, (2, 1, 0)))
    shift_one = own_depth(order(first_shift, (2, 1, 0)))
    vectors = order(jnp.stack([second_gain, second_shift, first_bias, second_bias]), (1, 2, 0))
    gain_two, shift_two = vectors[:1], vectors[1:2]
    vectors = own_half(jnp.concatenate([vectors[2:], upsample_bias[None]]))
    bias_one, bias_two, bias_up = [vectors[i : i + 1] for i in range(3)]

    def picks(group, groups):
        pick = group[:, None] == jnp.arange(128)[None, :]
        return jnp.concatenate([pick, jnp.roll(pick, groups, axis=1)]).astype(F32)

    lane = jnp.arange(depth)
    pick_one = picks(lane // k_own % nx * nzh + lane // (k_own * nx), G)
    lane = jnp.arange(channels)
    group = lane // (k_own * nx * nzl) * nx + lane // k_own % nx
    pick_two = picks(group, G)
    pick_own = picks(group[:half] + c * (G // ncol), G)

    parts = pl.pallas_call(
        functools.partial(conv_one_kernel, cols, image_rows, count),
        out_shape=jax.ShapeDtypeStruct((nzl, cols, half), BF16),
        in_specs=[SM] + [VM] * 6,
        out_specs=VM,
        scratch_shapes=[pltpu.VMEM(((nzl + 2) * cols, 3 * depth), BF16)],
        name="conv_one",
    )(at, quad, sums, gain_one, shift_one, pick_one, weights_one)
    parts = lax.all_to_all(parts, "zl", 0, 0, tiled=True)
    hidden, sums_two = pl.pallas_call(
        join_kernel,
        out_shape=(
            jax.ShapeDtypeStruct((cols, half), BF16),
            jax.ShapeDtypeStruct((8, 128), F32),
        ),
        in_specs=[VM] * 3,
        out_specs=(VM, VM),
        name="join_one",
    )(parts, bias_one, pick_own)

    stats = jnp.sum(sum_over(sums_two[:1], ("x", "zl", "col")), axis=0, keepdims=True)
    hidden, three, stats = lax.optimization_barrier((hidden, jnp.stack([up_row, own, down_row]), stats))
    stats = sum_over(stats, "zh")
    five = jnp.stack([shifted_rows(hidden, ROW, d) if d else hidden for d in range(-2, 3)])
    five = lax.all_gather(five, "col")
    three = lax.all_gather(three, "col", axis=1, tiled=True)
    residual = own_half(moved(three.reshape(3 * cols, channels), move))
    normed = pl.pallas_call(
        functools.partial(norm_kernel, image_rows, count),
        out_shape=jax.ShapeDtypeStruct((ncol, 5 * cols, half), BF16),
        in_specs=[SM] + [VM] * 5,
        out_specs=VM,
        name="norm_two",
    )(at, five, stats, gain_two, shift_two, pick_two)

    rows = 3
    block = pl.pallas_call(
        functools.partial(conv_two_kernel, cols, rows, image_rows),
        grid=(3,),
        out_shape=jax.ShapeDtypeStruct((rows * cols, half), BF16),
        in_specs=[SM, VM, VM, VM, weight_spec(weights, 0)],
        out_specs=VM,
        scratch_shapes=[
            pltpu.VMEM((3, (rows + 2) * cols, channels), BF16),
            pltpu.VMEM((rows * cols, half), F32),
        ],
        name="conv_two",
    )(at, normed, residual, bias_two, weights)
    block = lax.all_gather(block, "col")

    up = pl.pallas_call(
        functools.partial(conv_up_kernel, cols),
        grid=(3,),
        out_shape=jax.ShapeDtypeStruct((ncol, 2, cols, half), BF16),
        in_specs=[VM, VM, weight_spec(weights, 3)],
        out_specs=VM,
        scratch_shapes=[
            pltpu.VMEM((3, 3 * cols, channels), BF16),
            pltpu.VMEM((4, cols, half), F32),
            pltpu.VMEM((2, 2, 2 * cols, 128), F32),
        ],
        name="conv_up",
    )(block, bias_up, weights)
    up = lax.all_to_all(up, "col", 0, 0, tiled=True)
    return up.transpose(1, 2, 0, 3).reshape(2, cols, channels)


def solution(mesh):
    finer = Mesh(
        mesh.devices.reshape(mesh.shape["img"], 4, 8, 4, mesh.shape["col"]),
        IMG_ROW + ("col",),
    )
    in_specs = (
        P(IMG_ROW, "col", None),
        P(),
        P(),
        P(None, None, ROW, None),
        P(),
        P(),
        P(),
        P(None, None, ROW, None),
        P(),
        P(None, None, ROW, None),
        P(),
    )
    return jax.shard_map(
        on_device,
        mesh=finer,
        in_specs=in_specs,
        out_specs=P(IMG_ROW, "col", None),
        check_vma=False,
    )
```

```python
import functools

import jax
import jax.numpy as jnp
from jax import lax
from jax.experimental import pallas as pl
from jax.experimental.pallas import tpu as pltpu
from jax.sharding import Mesh
from jax.sharding import PartitionSpec as P

G = 32
EPS = 1e-06
F32, BF16 = jnp.float32, jnp.bfloat16
HIGHEST = lax.Precision.HIGHEST
ROW = ("x", "zh", "zl")
IMG_ROW = ("img",) + ROW


def sum_over(vector, axes):
    count = lax.axis_size(axes)
    sent = jnp.broadcast_to(vector, (count, vector.shape[1]))
    return lax.all_to_all(sent, axes, 0, 0, tiled=True)


def shifted_rows(values, axis, by):
    count = lax.axis_size(axis)
    pairs = [(i, i - by) for i in range(count) if 0 <= i - by < count]
    return lax.ppermute(values, axis, pairs)


def fetch(count, by):
    above = [(2 * (i - by), 2 * i) for i in range(by, count)]
    return above + [(2 * (i + by) + 1, 2 * i + 1) for i in range(count - by)]


def put_shifted(S, row, cols, y, lanes):
    at = pl.ds(row * cols, cols)
    column = lax.broadcasted_iota(jnp.int32, y.shape, 0)
    S[1, at, lanes] = y.astype(BF16)
    S[0, at, lanes] = jnp.where(column == 0, 0.0, pltpu.roll(y, 1, 0)).astype(BF16)
    S[2, at, lanes] = jnp.where(column == cols - 1, 0.0, pltpu.roll(y, cols - 1, 0)).astype(BF16)


def silu(u):
    return u / (1.0 + jnp.exp(-u))


def spread_stats(totals, pick, count, gain, shift):
    totals = jnp.broadcast_to(totals, (8, totals.shape[1]))
    spread = lax.dot_general(
        totals, pick, (((1,), (1,)), ((), ())), precision=HIGHEST, preferred_element_type=F32
    )
    width = gain.shape[1]
    mean = spread[:1, :width] / count
    var = spread[:1, width:] / count - mean * mean
    a = lax.rsqrt(var + EPS) * gain
    return a, shift - mean * a


def conv_one_kernel(cols, image_rows, count, at_ref, x_ref, gain_ref, shift_ref, pick_ref, w_ref, out_ref, S):
    quad, depth = x_ref.shape[0], x_ref.shape[4]
    totals = jnp.sum(w_ref[:, 9, :, :128].astype(F32).reshape(-1, 128), axis=0, keepdims=True)
    a, b = spread_stats(totals, pick_ref[...], count, gain_ref[...], shift_ref[...])
    first = at_ref[0] // quad * quad - 1
    column = lax.broadcasted_iota(jnp.int32, (cols, depth), 0)
    for i in range(quad + 2):
        member = min(max(i - 1, 0), quad - 1)
        slot = 0 if 1 <= i <= quad else 1
        x = jnp.concatenate([x_ref[member, h, slot] for h in range(x_ref.shape[1])], axis=0)
        y = silu(x.astype(F32) * a + b)
        if slot:
            y = jnp.where(jnp.logical_and(first + i >= 0, first + i < image_rows), y, 0.0)
        at = slice(i * cols, (i + 1) * cols)
        left = jnp.where(column == 0, 0.0, pltpu.roll(y, 1, 0))
        right = jnp.where(column == cols - 1, 0.0, pltpu.roll(y, cols - 1, 0))
        S[at, 0 * depth : 1 * depth] = left.astype(BF16)
        S[at, 1 * depth : 2 * depth] = y.astype(BF16)
        S[at, 2 * depth : 3 * depth] = right.astype(BF16)
    outs = out_ref.shape[2]
    total = jnp.zeros((quad * cols, outs), F32)
    for r in range(3):
        piece = jnp.concatenate([w_ref[:, 3 * r + k].reshape(depth, outs) for k in range(3)], axis=0)
        total += jnp.dot(S[r * cols : (r + quad) * cols, :], piece, preferred_element_type=F32)
    out_ref[...] = total.astype(BF16).reshape(quad, cols, outs)


def join_kernel(x_ref, bias_ref, pick_ref, out_ref, sums_ref):
    total = x_ref[0].astype(F32)
    for k in range(1, x_ref.shape[0]):
        total += x_ref[k].astype(F32)
    hidden = (total + bias_ref[...]).astype(BF16)
    out_ref[...] = hidden
    own = hidden.astype(F32)
    both = jnp.concatenate(
        [jnp.sum(own, axis=0, keepdims=True), jnp.sum(own * own, axis=0, keepdims=True)], axis=1
    )
    both = jnp.broadcast_to(both, (8, both.shape[1]))
    sums_ref[...] = jnp.dot(both, pick_ref[...], precision=HIGHEST, preferred_element_type=F32)


def norm_kernel(image_rows, count, at_ref, own_ref, far_ref, stats_ref, gain_ref, shift_ref, pick_ref, out_ref):
    totals = jnp.sum(stats_ref[...], axis=0, keepdims=True)
    a, b = spread_stats(totals, pick_ref[...], count, gain_ref[...], shift_ref[...])
    halves, cols, half = own_ref.shape
    for d in range(-2, 3):
        row = at_ref[0] + d
        inside = jnp.logical_and(row >= 0, row < image_rows)
        for h in range(halves):
            lanes = slice(h * half, (h + 1) * half)
            x = far_ref[int(d > 0), abs(d) - 1, h] if d else own_ref[h]
            y = silu(x.astype(F32) * a[:, lanes] + b[:, lanes])
            out_ref[h, (d + 2) * cols : (d + 3) * cols, :] = jnp.where(inside, y, 0.0).astype(BF16)


def conv_two_kernel(cols, rows, image_rows, at_ref, x_ref, res_ref, bias_ref, w_ref, out_ref, S, acc):
    t = pl.program_id(0)
    outs = acc.shape[1]

    @pl.when(t == 0)
    def _():
        for i in range(rows + 2):
            for h in range(2):
                y = x_ref[h, pl.ds(i * cols, cols), :].astype(F32)
                put_shifted(S, i, cols, y, slice(h * outs, (h + 1) * outs))
        acc[...] = jnp.broadcast_to(bias_ref[...], acc.shape)

    start = pl.multiple_of(t * cols, cols)
    total = acc[...]
    for k in range(3):
        piece = w_ref[:, k].reshape(-1, outs)
        total += jnp.dot(S[k, pl.ds(start, rows * cols), :], piece, preferred_element_type=F32)
    acc[...] = total

    @pl.when(t == 2)
    def _():
        first = at_ref[0] - rows // 2
        for i in range(rows):
            at = pl.ds(i * cols, cols)
            y = acc[at, :] + res_ref[at, :].astype(F32)
            inside = jnp.logical_and(first + i >= 0, first + i < image_rows)
            out_ref[at, :] = jnp.where(inside, y, 0.0).astype(BF16)


def conv_up_kernel(cols, x_ref, bias_ref, w_ref, out_ref, S, acc, full):
    t = pl.program_id(0)
    outs = acc.shape[2]

    @pl.when(t == 0)
    def _():
        for i in range(3):
            for h in range(2):
                y = x_ref[h, pl.ds(i * cols, cols), :].astype(F32)
                put_shifted(S, i, cols, y, slice(h * outs, (h + 1) * outs))
        acc[...] = jnp.broadcast_to(bias_ref[...][None], acc.shape)

    for p in range(2):
        start = pl.multiple_of(((t + 1 + p) // 2) * cols, cols)
        for q in range(2):
            total = acc[2 * p + q]
            for k in range(3):
                total += jnp.dot(
                    S[(k + 1 + q) // 2, pl.ds(start, cols), :],
                    w_ref[:, k].reshape(-1, outs),
                    preferred_element_type=F32,
                )
            acc[2 * p + q] = total

    @pl.when(t == 2)
    def _():
        for p in range(2):
            for q in range(2):
                for k in range(2):
                    lanes = slice(k * 128, (k + 1) * 128)
                    full[p, k, pl.ds(q, cols, stride=2), :] = acc[2 * p + q][:, lanes]
            for k in range(2):
                for half in range(2):
                    out_ref[half, p, :, k * 128 : (k + 1) * 128] = full[
                        p, k, half * cols : (half + 1) * cols, :
                    ].astype(BF16)


VM = pl.BlockSpec(memory_space=pltpu.VMEM)
SM = pl.BlockSpec(memory_space=pltpu.SMEM)


def weight_spec(gathered, base):
    n, _, rows, outs = gathered.shape
    return pl.BlockSpec((n, 3, rows, outs), lambda t: (0, base + t, 0, 0))


def on_device(
    features,
    first_gain,
    first_shift,
    first_weight,
    first_bias,
    second_gain,
    second_shift,
    second_weight,
    second_bias,
    upsample_weight,
    upsample_bias,
):
    _, breadth, channels = features.shape
    nx, nzh, nzl, ncol = (lax.axis_size(axis) for axis in ("x", "zh", "zl", "col"))
    nz = nzh * nzl
    k_own = first_weight.shape[2]
    cols = breadth * ncol
    half = channels // ncol
    depth = channels // nzl
    image_rows = nx * nz
    per_group = channels // G
    count = image_rows * cols * per_group
    c = lax.axis_index("col")
    zl = lax.axis_index("zl")
    at = lax.axis_index(ROW).astype(jnp.int32)[None]

    def order(v, axes):
        v = v.reshape(-1, nx, nzh, nzl, k_own).transpose(0, *[k + 1 for k in axes], 4)
        return v.reshape(-1, channels)

    place = lax.broadcasted_iota(jnp.int32, (channels, channels), 1)
    natural = lax.broadcasted_iota(jnp.int32, (channels, channels), 0)
    k, x = place % k_own, place // k_own % nx
    line = place // (k_own * nx)
    source = (x * nz + line) * k_own + k
    move = (natural == source).astype(BF16)
    source = (x * nz + line % nzh * nzl + line // nzh) * k_own + k
    move_one = (natural == source).astype(BF16)

    def moved(v, by):
        return jnp.dot(v, by, preferred_element_type=F32).astype(BF16)

    def own_half(v):
        return lax.dynamic_slice_in_dim(v, c * half, half, v.ndim - 1)

    taps = 9 * k_own
    hold = moved(
        jnp.concatenate([first_weight.reshape(taps, channels), second_weight.reshape(taps, channels)]),
        move,
    )
    hold = jnp.concatenate([hold, upsample_weight.reshape(taps, channels)])
    hold = own_half(hold).reshape(1, 27, k_own, half)
    hold = lax.all_to_all(jnp.broadcast_to(hold, (nx, 27, k_own, half)), "x", 0, 0, tiled=True)
    hold = hold.transpose(1, 0, 2, 3).reshape(27, nx * k_own, half)
    weights = lax.all_gather(hold[9:], ("zh", "zl"))
    hold_one = hold[:9]

    own = features[0]
    wide = own.astype(F32)
    chan = lax.broadcasted_iota(jnp.int32, (channels, G), 0) // per_group
    member = (chan == lax.broadcasted_iota(jnp.int32, (channels, G), 1)).astype(F32)
    sums = jnp.stack([jnp.sum(wide, axis=0), jnp.sum(wide * wide, axis=0)])
    sums = jnp.dot(sums, member, precision=HIGHEST).reshape(1, 2 * G)
    sums = jnp.pad(sums, ((0, 0), (0, 128 - 2 * G)))
    sums = jnp.sum(sum_over(sums, ("x", "zl", "col")), axis=0, keepdims=True)
    high = lax.reduce_precision(sums, 8, 7)
    low = lax.reduce_precision(sums - high, 8, 7)
    terms = jnp.concatenate([high, low, sums - high - low]).astype(BF16)
    terms = jnp.pad(terms, ((0, nx * k_own - 3), (0, half - 128)))
    weights_one = lax.all_gather(jnp.concatenate([hold_one, terms[None]]), "zh")

    last = nx * nz - 1
    pairs = [(i, i + 1) for i in range(nzl - 1, last, nzl)] + [(i, i - 1) for i in range(nzl, last, nzl)]
    edge = lax.ppermute(own, ROW, pairs)
    sent = moved(jnp.concatenate([own, edge]), move_one)
    sent = sent.reshape(2, breadth, nzl, depth).transpose(2, 0, 1, 3)
    sent = jnp.broadcast_to(sent[:, None], (nzl, ncol, 2, breadth, depth))
    sent = sent.reshape(nzl * ncol, 2, breadth, depth)
    quad = lax.all_to_all(sent, ("zl", "col"), 0, 0, tiled=True)

    quad = quad.reshape(nzl, ncol, 2, breadth, depth)

    def own_depth(v):
        return lax.dynamic_slice_in_dim(v, zl * depth, depth, 1)

    gain_one = own_depth(order(first_gain, (2, 1, 0)))
    shift_one = own_depth(order(first_shift, (2, 1, 0)))
    vectors = order(jnp.stack([second_gain, second_shift, first_bias, second_bias]), (1, 2, 0))
    gain_two, shift_two = vectors[:1], vectors[1:2]
    vectors = own_half(jnp.concatenate([vectors[2:], upsample_bias[None]]))
    bias_one, bias_two, bias_up = [vectors[i : i + 1] for i in range(3)]

    def picks(group, groups):
        pick = group[:, None] == jnp.arange(128)[None, :]
        return jnp.concatenate([pick, jnp.roll(pick, groups, axis=1)]).astype(F32)

    lane = jnp.arange(depth)
    pick_one = picks(lane // k_own % nx * nzh + lane // (k_own * nx), G)
    lane = jnp.arange(channels)
    group = lane // (k_own * nx * nzl) * nx + lane // k_own % nx
    pick_two = picks(group, G)
    pick_own = picks(group[:half] + c * (G // ncol), G)

    parts = pl.pallas_call(
        functools.partial(conv_one_kernel, cols, image_rows, count),
        out_shape=jax.ShapeDtypeStruct((nzl, cols, half), BF16),
        in_specs=[SM] + [VM] * 5,
        out_specs=VM,
        scratch_shapes=[pltpu.VMEM(((nzl + 2) * cols, 3 * depth), BF16)],
        name="conv_one",
    )(at, quad, gain_one, shift_one, pick_one, weights_one)
    parts, own = lax.optimization_barrier((parts, own))
    parts = lax.all_to_all(parts, "zl", 0, 0, tiled=True)
    three = jnp.stack([shifted_rows(own, ROW, -1), own, shifted_rows(own, ROW, 1)])
    hidden, sums_two = pl.pallas_call(
        join_kernel,
        out_shape=(
            jax.ShapeDtypeStruct((cols, half), BF16),
            jax.ShapeDtypeStruct((8, 128), F32),
        ),
        in_specs=[VM] * 3,
        out_specs=(VM, VM),
        name="join_one",
    )(parts, bias_one, pick_own)

    stats = jnp.sum(sum_over(sums_two[:1], ("x", "zl", "col")), axis=0, keepdims=True)
    both = lax.all_gather(hidden, "col")
    stats = sum_over(stats, "zh")
    far = jnp.stack([lax.ppermute(both, ROW + ("col",), fetch(nx * nz, d)) for d in (1, 2)])
    far, three = lax.optimization_barrier((far, three))
    far = lax.all_gather(far, "col")
    three = lax.all_gather(three, "col", axis=1, tiled=True)
    residual = own_half(moved(three.reshape(3 * cols, channels), move))
    normed = pl.pallas_call(
        functools.partial(norm_kernel, image_rows, count),
        out_shape=jax.ShapeDtypeStruct((ncol, 5 * cols, half), BF16),
        in_specs=[SM] + [VM] * 6,
        out_specs=VM,
        name="norm_two",
    )(at, both, far, stats, gain_two, shift_two, pick_two)

    rows = 3
    block = pl.pallas_call(
        functools.partial(conv_two_kernel, cols, rows, image_rows),
        grid=(3,),
        out_shape=jax.ShapeDtypeStruct((rows * cols, half), BF16),
        in_specs=[SM, VM, VM, VM, weight_spec(weights, 0)],
        out_specs=VM,
        scratch_shapes=[
            pltpu.VMEM((3, (rows + 2) * cols, channels), BF16),
            pltpu.VMEM((rows * cols, half), F32),
        ],
        name="conv_two",
    )(at, normed, residual, bias_two, weights)
    block = lax.all_gather(block, "col")

    up = pl.pallas_call(
        functools.partial(conv_up_kernel, cols),
        grid=(3,),
        out_shape=jax.ShapeDtypeStruct((ncol, 2, cols, half), BF16),
        in_specs=[VM, VM, weight_spec(weights, 3)],
        out_specs=VM,
        scratch_shapes=[
            pltpu.VMEM((3, 3 * cols, channels), BF16),
            pltpu.VMEM((4, cols, half), F32),
            pltpu.VMEM((2, 2, 2 * cols, 128), F32),
        ],
        name="conv_up",
    )(block, bias_up, weights)
    up = lax.all_to_all(up, "col", 0, 0, tiled=True)
    return up.transpose(1, 2, 0, 3).reshape(2, cols, channels)


def solution(mesh):
    finer = Mesh(
        mesh.devices.reshape(mesh.shape["img"], 4, 8, 4, mesh.shape["col"]),
        IMG_ROW + ("col",),
    )
    in_specs = (
        P(IMG_ROW, "col", None),
        P(),
        P(),
        P(None, None, ROW, None),
        P(),
        P(),
        P(),
        P(None, None, ROW, None),
        P(),
        P(None, None, ROW, None),
        P(),
    )

    return jax.shard_map(
        on_device,
        mesh=finer,
        in_specs=in_specs,
        out_specs=P(IMG_ROW, "col", None),
        check_vma=False,
    )
```

```python
import functools

import jax
import jax.numpy as jnp
from jax import lax
from jax.experimental import pallas as pl
from jax.experimental.pallas import tpu as pltpu
from jax.sharding import Mesh
from jax.sharding import PartitionSpec as P

G = 32
EPS = 1e-06
F32, BF16 = jnp.float32, jnp.bfloat16
HIGHEST = lax.Precision.HIGHEST
ROW = ("x", "zh", "zl")
IMG_ROW = ("img",) + ROW


def sum_over(vector, axes):
    count = lax.axis_size(axes)
    sent = jnp.broadcast_to(vector, (count, vector.shape[1]))
    return lax.all_to_all(sent, axes, 0, 0, tiled=True)


def shifted_rows(values, axis, by):
    count = lax.axis_size(axis)
    pairs = [(i, i - by) for i in range(count) if 0 <= i - by < count]
    return lax.ppermute(values, axis, pairs)


def fetch(count, by):
    above = [(2 * (i - by), 2 * i) for i in range(by, count)]
    return above + [(2 * (i + by) + 1, 2 * i + 1) for i in range(count - by)]


def put_shifted(S, row, cols, y, lanes):
    at = pl.ds(row * cols, cols)
    column = lax.broadcasted_iota(jnp.int32, y.shape, 0)
    S[1, at, lanes] = y.astype(BF16)
    S[0, at, lanes] = jnp.where(column == 0, 0.0, pltpu.roll(y, 1, 0)).astype(BF16)
    S[2, at, lanes] = jnp.where(column == cols - 1, 0.0, pltpu.roll(y, cols - 1, 0)).astype(BF16)


def silu(u):
    return u / (1.0 + jnp.exp(-u))


def spread_stats(totals, pick, count, gain, shift):
    totals = jnp.broadcast_to(totals, (8, totals.shape[1]))
    spread = lax.dot_general(
        totals, pick, (((1,), (1,)), ((), ())), precision=HIGHEST, preferred_element_type=F32
    )
    width = gain.shape[1]
    mean = spread[:1, :width] / count
    var = spread[:1, width:] / count - mean * mean
    a = lax.rsqrt(var + EPS) * gain
    return a, shift - mean * a


def conv_one_kernel(cols, image_rows, count, at_ref, x_ref, gain_ref, shift_ref, pick_ref, w_ref, out_ref, S):
    quad, depth = x_ref.shape[0], x_ref.shape[4]
    totals = jnp.sum(w_ref[:, 9, :, :128].astype(F32).reshape(-1, 128), axis=0, keepdims=True)
    a, b = spread_stats(totals, pick_ref[...], count, gain_ref[...], shift_ref[...])
    first = at_ref[0] // quad * quad - 1
    column = lax.broadcasted_iota(jnp.int32, (cols, depth), 0)
    for i in range(quad + 2):
        member = min(max(i - 1, 0), quad - 1)
        slot = 0 if 1 <= i <= quad else 1
        x = jnp.concatenate([x_ref[member, h, slot] for h in range(x_ref.shape[1])], axis=0)
        y = silu(x.astype(F32) * a + b)
        if slot:
            y = jnp.where(jnp.logical_and(first + i >= 0, first + i < image_rows), y, 0.0)
        at = slice(i * cols, (i + 1) * cols)
        left = jnp.where(column == 0, 0.0, pltpu.roll(y, 1, 0))
        right = jnp.where(column == cols - 1, 0.0, pltpu.roll(y, cols - 1, 0))
        S[at, 0 * depth : 1 * depth] = left.astype(BF16)
        S[at, 1 * depth : 2 * depth] = y.astype(BF16)
        S[at, 2 * depth : 3 * depth] = right.astype(BF16)
    outs = out_ref.shape[2]
    total = jnp.zeros((quad * cols, outs), F32)
    for r in range(3):
        piece = jnp.concatenate([w_ref[:, 3 * r + k].reshape(depth, outs) for k in range(3)], axis=0)
        total += jnp.dot(S[r * cols : (r + quad) * cols, :], piece, preferred_element_type=F32)
    out_ref[...] = total.astype(BF16).reshape(quad, cols, outs)


def join_kernel(x_ref, bias_ref, pick_ref, out_ref, sums_ref):
    total = x_ref[0].astype(F32)
    for k in range(1, x_ref.shape[0]):
        total += x_ref[k].astype(F32)
    hidden = (total + bias_ref[...]).astype(BF16)
    out_ref[...] = hidden
    own = hidden.astype(F32)
    both = jnp.concatenate(
        [jnp.sum(own, axis=0, keepdims=True), jnp.sum(own * own, axis=0, keepdims=True)], axis=1
    )
    both = jnp.broadcast_to(both, (8, both.shape[1]))
    sums_ref[...] = jnp.dot(both, pick_ref[...], precision=HIGHEST, preferred_element_type=F32)


def norm_kernel(image_rows, count, at_ref, own_ref, far_ref, stats_ref, gain_ref, shift_ref, pick_ref, out_ref):
    totals = jnp.sum(stats_ref[...], axis=0, keepdims=True)
    a, b = spread_stats(totals, pick_ref[...], count, gain_ref[...], shift_ref[...])
    halves, cols, half = own_ref.shape
    for d in range(-2, 3):
        row = at_ref[0] + d
        inside = jnp.logical_and(row >= 0, row < image_rows)
        for h in range(halves):
            lanes = slice(h * half, (h + 1) * half)
            x = far_ref[int(d > 0), abs(d) - 1, h] if d else own_ref[h]
            y = silu(x.astype(F32) * a[:, lanes] + b[:, lanes])
            out_ref[h, (d + 2) * cols : (d + 3) * cols, :] = jnp.where(inside, y, 0.0).astype(BF16)


def fetch_weights(w_ref, base, held, arrived):
    copies = [
        pltpu.make_async_copy(w_ref.at[:, pl.ds(base + 3 * r, 3)], held.at[r], arrived.at[r])
        for r in range(3)
    ]
    for copy in copies:
        copy.start()
    return copies


def conv_two_kernel(cols, rows, image_rows, at_ref, x_ref, res_ref, bias_ref, w_ref, out_ref, S, held, arrived):
    copies = fetch_weights(w_ref, 0, held, arrived)
    outs = out_ref.shape[1]
    for i in range(rows + 2):
        for h in range(2):
            y = x_ref[h, i * cols : (i + 1) * cols, :].astype(F32)
            put_shifted(S, i, cols, y, slice(h * outs, (h + 1) * outs))
    total = jnp.broadcast_to(bias_ref[...], out_ref.shape)
    for r in range(3):
        copies[r].wait()
        for k in range(3):
            piece = held[r, :, k].reshape(-1, outs)
            total += jnp.dot(
                S[k, r * cols : (r + rows) * cols, :], piece, preferred_element_type=F32
            )
    first = at_ref[0] - rows // 2
    for i in range(rows):
        at = slice(i * cols, (i + 1) * cols)
        y = total[at] + res_ref[at, :].astype(F32)
        inside = jnp.logical_and(first + i >= 0, first + i < image_rows)
        out_ref[at, :] = jnp.where(inside, y, 0.0).astype(BF16)


def conv_up_kernel(cols, at_ref, x_ref, bias_ref, w_ref, out_ref, S, full, held, arrived):
    copies = fetch_weights(w_ref, 9, held, arrived)
    outs = out_ref.shape[2]
    part = out_ref.shape[1] // 2
    for i in range(3):
        for h in range(2):
            y = x_ref[h, i * cols : (i + 1) * cols, :].astype(F32)
            put_shifted(S, i, cols, y, slice(h * outs, (h + 1) * outs))
    begin = at_ref[0] * part
    totals = [jnp.broadcast_to(bias_ref[...], (part, outs)) for _ in range(4)]
    for r in range(3):
        copies[r].wait()
        for k in range(3):
            piece = held[r, :, k].reshape(-1, outs)
            for p in range(2):
                start = pl.multiple_of((r + 1 + p) // 2 * cols + begin, part)
                for q in range(2):
                    totals[2 * p + q] += jnp.dot(
                        S[(k + 1 + q) // 2, pl.ds(start, part), :], piece, preferred_element_type=F32
                    )
    for p in range(2):
        for k in range(2):
            lanes = slice(k * 128, (k + 1) * 128)
            for q in range(2):
                full[p, k, pl.ds(q, part, stride=2), :] = totals[2 * p + q][:, lanes]
            out_ref[p, :, lanes] = full[p, k].astype(BF16)


def grant(mebibytes):
    return pltpu.CompilerParams(vmem_limit_bytes=mebibytes << 20)


VM = pl.BlockSpec(memory_space=pltpu.VMEM)
SM = pl.BlockSpec(memory_space=pltpu.SMEM)
HB = pl.BlockSpec(memory_space=pltpu.HBM)


def on_device(
    features,
    first_gain,
    first_shift,
    first_weight,
    first_bias,
    second_gain,
    second_shift,
    second_weight,
    second_bias,
    upsample_weight,
    upsample_bias,
):
    _, breadth, channels = features.shape
    nx, nzh, nzl, ncol = (lax.axis_size(axis) for axis in ("x", "zh", "zl", "col"))
    nz = nzh * nzl
    k_own = first_weight.shape[2]
    cols = breadth * ncol
    half = channels // ncol
    depth = channels // nzl
    image_rows = nx * nz
    per_group = channels // G
    count = image_rows * cols * per_group
    c = lax.axis_index("col")
    zl = lax.axis_index("zl")
    at = lax.axis_index(ROW).astype(jnp.int32)[None]

    def order(v, axes):
        v = v.reshape(-1, nx, nzh, nzl, k_own).transpose(0, *[k + 1 for k in axes], 4)
        return v.reshape(-1, channels)

    place = lax.broadcasted_iota(jnp.int32, (channels, channels), 1)
    natural = lax.broadcasted_iota(jnp.int32, (channels, channels), 0)
    k, x = place % k_own, place // k_own % nx
    line = place // (k_own * nx)
    source = (x * nz + line) * k_own + k
    move = (natural == source).astype(BF16)
    source = (x * nz + line % nzh * nzl + line // nzh) * k_own + k
    move_one = (natural == source).astype(BF16)

    def moved(v, by):
        return jnp.dot(v, by, preferred_element_type=F32).astype(BF16)

    def own_half(v):
        return lax.dynamic_slice_in_dim(v, c * half, half, v.ndim - 1)

    taps = 9 * k_own
    hold = moved(
        jnp.concatenate([first_weight.reshape(taps, channels), second_weight.reshape(taps, channels)]),
        move,
    )
    hold = jnp.concatenate([hold, upsample_weight.reshape(taps, channels)])
    hold = own_half(hold).reshape(1, 27, k_own, half)
    hold = lax.all_to_all(jnp.broadcast_to(hold, (nx, 27, k_own, half)), "x", 0, 0, tiled=True)
    hold = hold.transpose(1, 0, 2, 3).reshape(27, nx * k_own, half)
    weights = lax.all_gather(hold[9:], ("zh", "zl"))
    hold_one = hold[:9]

    own = features[0]
    wide = own.astype(F32)
    chan = lax.broadcasted_iota(jnp.int32, (channels, G), 0) // per_group
    member = (chan == lax.broadcasted_iota(jnp.int32, (channels, G), 1)).astype(F32)
    sums = jnp.stack([jnp.sum(wide, axis=0), jnp.sum(wide * wide, axis=0)])
    sums = jnp.dot(sums, member, precision=HIGHEST).reshape(1, 2 * G)
    sums = jnp.pad(sums, ((0, 0), (0, 128 - 2 * G)))
    sums = jnp.sum(sum_over(sums, ("x", "zl", "col")), axis=0, keepdims=True)
    high = lax.reduce_precision(sums, 8, 7)
    low = lax.reduce_precision(sums - high, 8, 7)
    terms = jnp.concatenate([high, low, sums - high - low]).astype(BF16)
    terms = jnp.pad(terms, ((0, nx * k_own - 3), (0, half - 128)))
    weights_one = lax.all_gather(jnp.concatenate([hold_one, terms[None]]), "zh")

    last = nx * nz - 1
    pairs = [(i, i + 1) for i in range(nzl - 1, last, nzl)] + [(i, i - 1) for i in range(nzl, last, nzl)]
    edge = lax.ppermute(own, ROW, pairs)
    sent = moved(jnp.concatenate([own, edge]), move_one)
    sent = sent.reshape(2, breadth, nzl, depth).transpose(2, 0, 1, 3)
    sent = jnp.broadcast_to(sent[:, None], (nzl, ncol, 2, breadth, depth))
    sent = sent.reshape(nzl * ncol, 2, breadth, depth)
    quad = lax.all_to_all(sent, ("zl", "col"), 0, 0, tiled=True)

    quad = quad.reshape(nzl, ncol, 2, breadth, depth)

    def own_depth(v):
        return lax.dynamic_slice_in_dim(v, zl * depth, depth, 1)

    gain_one = own_depth(order(first_gain, (2, 1, 0)))
    shift_one = own_depth(order(first_shift, (2, 1, 0)))
    vectors = order(jnp.stack([second_gain, second_shift, first_bias, second_bias]), (1, 2, 0))
    gain_two, shift_two = vectors[:1], vectors[1:2]
    vectors = own_half(jnp.concatenate([vectors[2:], upsample_bias[None]]))
    bias_one, bias_two, bias_up = [vectors[i : i + 1] for i in range(3)]

    def picks(group, groups):
        pick = group[:, None] == jnp.arange(128)[None, :]
        return jnp.concatenate([pick, jnp.roll(pick, groups, axis=1)]).astype(F32)

    lane = jnp.arange(depth)
    pick_one = picks(lane // k_own % nx * nzh + lane // (k_own * nx), G)
    lane = jnp.arange(channels)
    group = lane // (k_own * nx * nzl) * nx + lane // k_own % nx
    pick_two = picks(group, G)
    pick_own = picks(group[:half] + c * (G // ncol), G)

    parts = pl.pallas_call(
        functools.partial(conv_one_kernel, cols, image_rows, count),
        out_shape=jax.ShapeDtypeStruct((nzl, cols, half), BF16),
        in_specs=[SM] + [VM] * 5,
        out_specs=VM,
        scratch_shapes=[pltpu.VMEM(((nzl + 2) * cols, 3 * depth), BF16)],
        compiler_params=grant(16),
        name="conv_one",
    )(at, quad, gain_one, shift_one, pick_one, weights_one)
    parts, own = lax.optimization_barrier((parts, own))
    parts = lax.all_to_all(parts, "zl", 0, 0, tiled=True)
    three = jnp.stack([shifted_rows(own, ROW, -1), own, shifted_rows(own, ROW, 1)])
    hidden, sums_two = pl.pallas_call(
        join_kernel,
        out_shape=(
            jax.ShapeDtypeStruct((cols, half), BF16),
            jax.ShapeDtypeStruct((8, 128), F32),
        ),
        in_specs=[VM] * 3,
        out_specs=(VM, VM),
        compiler_params=grant(8),
        name="join_one",
    )(parts, bias_one, pick_own)

    stats = jnp.sum(sum_over(sums_two[:1], ("x", "zl", "col")), axis=0, keepdims=True)
    both = lax.all_gather(hidden, "col")
    three = lax.all_gather(three, "col", axis=1, tiled=True)
    residual = own_half(moved(three.reshape(3 * cols, channels), move))
    stats, both, residual = lax.optimization_barrier((stats, both, residual))
    stats = sum_over(stats, "zh")
    far = jnp.stack([lax.ppermute(both, ROW + ("col",), fetch(nx * nz, d)) for d in (1, 2)])
    far = lax.all_gather(far, "col")
    normed = pl.pallas_call(
        functools.partial(norm_kernel, image_rows, count),
        out_shape=jax.ShapeDtypeStruct((ncol, 5 * cols, half), BF16),
        in_specs=[SM] + [VM] * 6,
        out_specs=VM,
        compiler_params=grant(12),
        name="norm_two",
    )(at, both, far, stats, gain_two, shift_two, pick_two)

    rows = 3
    held = [
        pltpu.VMEM((3, weights.shape[0], 3) + weights.shape[2:], BF16),
        pltpu.SemaphoreType.DMA((3,)),
    ]
    block = pl.pallas_call(
        functools.partial(conv_two_kernel, cols, rows, image_rows),
        out_shape=jax.ShapeDtypeStruct((rows * cols, half), BF16),
        in_specs=[SM, VM, VM, VM, HB],
        out_specs=VM,
        scratch_shapes=[pltpu.VMEM((3, (rows + 2) * cols, channels), BF16)] + held,
        compiler_params=grant(58),
        name="conv_two",
    )(at, normed, residual, bias_two, weights)
    block = lax.all_gather(block, "col")

    def up(part):
        return pl.pallas_call(
            functools.partial(conv_up_kernel, cols),
            out_shape=jax.ShapeDtypeStruct((2, cols, half), BF16),
            in_specs=[SM, VM, VM, HB],
            out_specs=VM,
            scratch_shapes=[
                pltpu.VMEM((3, 3 * cols, channels), BF16),
                pltpu.VMEM((2, 2, cols, 128), F32),
            ]
            + held,
            compiler_params=grant(58),
            cost_estimate=pl.CostEstimate(flops=4_000_000_000, bytes_accessed=3 << 20, transcendentals=0),
            name="conv_up",
        )(part, block, bias_up, weights)

    mine = c.astype(jnp.int32)[None]
    theirs = lax.ppermute(up(1 - mine), "col", [(0, 1), (1, 0)])
    ours = up(mine)
    return jnp.where(
        c == 0, jnp.concatenate([ours, theirs], axis=2), jnp.concatenate([theirs, ours], axis=2)
    )


def solution(mesh):
    finer = Mesh(
        mesh.devices.reshape(mesh.shape["img"], 4, 8, 4, mesh.shape["col"]),
        IMG_ROW + ("col",),
    )
    in_specs = (
        P(IMG_ROW, "col", None),
        P(),
        P(),
        P(None, None, ROW, None),
        P(),
        P(),
        P(),
        P(None, None, ROW, None),
        P(),
        P(None, None, ROW, None),
        P(),
    )

    return jax.shard_map(
        on_device,
        mesh=finer,
        in_specs=in_specs,
        out_specs=P(IMG_ROW, "col", None),
        check_vma=False,
    )
```

```python
import functools

import jax
import jax.numpy as jnp
from jax import lax
from jax.experimental import pallas as pl
from jax.experimental.pallas import tpu as pltpu
from jax.sharding import Mesh
from jax.sharding import PartitionSpec as P

G = 32
EPS = 1e-06
F32, BF16 = jnp.float32, jnp.bfloat16
HIGHEST = lax.Precision.HIGHEST
ROW = ("x", "zh", "zl")
IMG_ROW = ("img",) + ROW


def sum_over(vector, axes):
    count = lax.axis_size(axes)
    sent = jnp.broadcast_to(vector, (count, vector.shape[1]))
    return lax.all_to_all(sent, axes, 0, 0, tiled=True)


def shifted_rows(values, axis, by):
    count = lax.axis_size(axis)
    pairs = [(i, i - by) for i in range(count) if 0 <= i - by < count]
    return lax.ppermute(values, axis, pairs)


def fetch(count, by):
    above = [(2 * (i - by), 2 * i) for i in range(by, count)]
    return above + [(2 * (i + by) + 1, 2 * i + 1) for i in range(count - by)]


def put_shifted(S, row, cols, y, lanes):
    at = pl.ds(row * cols, cols)
    column = lax.broadcasted_iota(jnp.int32, y.shape, 0)
    S[1, at, lanes] = y.astype(BF16)
    S[0, at, lanes] = jnp.where(column == 0, 0.0, pltpu.roll(y, 1, 0)).astype(BF16)
    S[2, at, lanes] = jnp.where(column == cols - 1, 0.0, pltpu.roll(y, cols - 1, 0)).astype(BF16)


def silu(u):
    return u / (1.0 + jnp.exp(-u))


def spread_stats(totals, pick, count, gain, shift):
    totals = jnp.broadcast_to(totals, (8, totals.shape[1]))
    spread = lax.dot_general(
        totals, pick, (((1,), (1,)), ((), ())), precision=HIGHEST, preferred_element_type=F32
    )
    width = gain.shape[1]
    mean = spread[:1, :width] / count
    var = spread[:1, width:] / count - mean * mean
    a = lax.rsqrt(var + EPS) * gain
    return a, shift - mean * a


def conv_one_kernel(cols, image_rows, count, at_ref, x_ref, gain_ref, shift_ref, pick_ref, w_ref, out_ref, S):
    quad, depth = x_ref.shape[0], x_ref.shape[4]
    totals = jnp.sum(w_ref[:, 9, :, :128].astype(F32).reshape(-1, 128), axis=0, keepdims=True)
    a, b = spread_stats(totals, pick_ref[...], count, gain_ref[...], shift_ref[...])
    first = at_ref[0] // quad * quad - 1
    column = lax.broadcasted_iota(jnp.int32, (cols, depth), 0)
    for i in range(quad + 2):
        member = min(max(i - 1, 0), quad - 1)
        slot = 0 if 1 <= i <= quad else 1
        x = jnp.concatenate([x_ref[member, h, slot] for h in range(x_ref.shape[1])], axis=0)
        y = silu(x.astype(F32) * a + b)
        if slot:
            y = jnp.where(jnp.logical_and(first + i >= 0, first + i < image_rows), y, 0.0)
        at = slice(i * cols, (i + 1) * cols)
        left = jnp.where(column == 0, 0.0, pltpu.roll(y, 1, 0))
        right = jnp.where(column == cols - 1, 0.0, pltpu.roll(y, cols - 1, 0))
        S[at, 0 * depth : 1 * depth] = left.astype(BF16)
        S[at, 1 * depth : 2 * depth] = y.astype(BF16)
        S[at, 2 * depth : 3 * depth] = right.astype(BF16)
    outs = out_ref.shape[2]
    total = jnp.zeros((quad * cols, outs), F32)
    for r in range(3):
        piece = jnp.concatenate([w_ref[:, 3 * r + k].reshape(depth, outs) for k in range(3)], axis=0)
        total += jnp.dot(S[r * cols : (r + quad) * cols, :], piece, preferred_element_type=F32)
    out_ref[...] = total.astype(BF16).reshape(quad, cols, outs)


def join_kernel(x_ref, bias_ref, pick_ref, out_ref, sums_ref):
    total = x_ref[0].astype(F32)
    for k in range(1, x_ref.shape[0]):
        total += x_ref[k].astype(F32)
    hidden = (total + bias_ref[...]).astype(BF16)
    out_ref[...] = hidden
    own = hidden.astype(F32)
    both = jnp.concatenate(
        [jnp.sum(own, axis=0, keepdims=True), jnp.sum(own * own, axis=0, keepdims=True)], axis=1
    )
    both = jnp.broadcast_to(both, (8, both.shape[1]))
    sums_ref[...] = jnp.dot(both, pick_ref[...], precision=HIGHEST, preferred_element_type=F32)


def norm_kernel(image_rows, count, at_ref, own_ref, far_ref, stats_ref, gain_ref, shift_ref, pick_ref, out_ref):
    totals = jnp.sum(stats_ref[...], axis=0, keepdims=True)
    a, b = spread_stats(totals, pick_ref[...], count, gain_ref[...], shift_ref[...])
    halves, cols, half = own_ref.shape
    for d in range(-2, 3):
        row = at_ref[0] + d
        inside = jnp.logical_and(row >= 0, row < image_rows)
        for h in range(halves):
            lanes = slice(h * half, (h + 1) * half)
            x = far_ref[int(d > 0), abs(d) - 1, h] if d else own_ref[h]
            y = silu(x.astype(F32) * a[:, lanes] + b[:, lanes])
            out_ref[h, (d + 2) * cols : (d + 3) * cols, :] = jnp.where(inside, y, 0.0).astype(BF16)


def fetch_weights(w_ref, base, held, arrived):
    copies = [
        pltpu.make_async_copy(w_ref.at[:, base + t], held.at[t], arrived.at[t]) for t in range(9)
    ]
    for copy in copies:
        copy.start()
    return copies


def conv_two_kernel(cols, rows, image_rows, at_ref, x_ref, res_ref, bias_ref, w_ref, out_ref, S, held, arrived):
    copies = fetch_weights(w_ref, 0, held, arrived)
    outs = out_ref.shape[1]
    for i in range(rows + 2):
        for h in range(2):
            y = x_ref[h, i * cols : (i + 1) * cols, :].astype(F32)
            put_shifted(S, i, cols, y, slice(h * outs, (h + 1) * outs))
    total = jnp.broadcast_to(bias_ref[...], out_ref.shape)
    for r in range(3):
        for k in range(3):
            copies[3 * r + k].wait()
            piece = held[3 * r + k].reshape(-1, outs)
            total += jnp.dot(
                S[k, r * cols : (r + rows) * cols, :], piece, preferred_element_type=F32
            )
    first = at_ref[0] - rows // 2
    for i in range(rows):
        at = slice(i * cols, (i + 1) * cols)
        y = total[at] + res_ref[at, :].astype(F32)
        inside = jnp.logical_and(first + i >= 0, first + i < image_rows)
        out_ref[at, :] = jnp.where(inside, y, 0.0).astype(BF16)


def conv_up_kernel(cols, at_ref, x_ref, bias_ref, w_ref, mine_ref, theirs_ref, S, full, held, arrived):
    copies = fetch_weights(w_ref, 9, held, arrived)
    outs = mine_ref.shape[2]
    for i in range(3):
        for h in range(2):
            y = x_ref[h, i * cols : (i + 1) * cols, :].astype(F32)
            put_shifted(S, i, cols, y, slice(h * outs, (h + 1) * outs))
    total = jnp.broadcast_to(bias_ref[...], (4 * cols, outs))
    for r in range(3):
        for k in range(3):
            copies[3 * r + k].wait()
            piece = held[3 * r + k].reshape(-1, outs)
            phases = []
            for p in range(2):
                start = (r + 1 + p) // 2 * cols
                phases += [S[(k + 1 + q) // 2, start : start + cols, :] for q in range(2)]
            total += jnp.dot(jnp.concatenate(phases), piece, preferred_element_type=F32)
    mine = pl.multiple_of(at_ref[0] * cols, cols)
    theirs = pl.multiple_of((1 - at_ref[0]) * cols, cols)
    for p in range(2):
        for k in range(2):
            lanes = slice(k * 128, (k + 1) * 128)
            for q in range(2):
                phase = (2 * p + q) * cols
                full[p, k, pl.ds(q, cols, stride=2), :] = total[phase : phase + cols, lanes]
            mine_ref[p, :, lanes] = full[p, k, pl.ds(mine, cols), :].astype(BF16)
            theirs_ref[p, :, lanes] = full[p, k, pl.ds(theirs, cols), :].astype(BF16)


def sides_kernel(at_ref, mine_ref, theirs_ref, out_ref):
    outs = mine_ref.shape[2]
    for k, first, second in ((0, mine_ref, theirs_ref), (1, theirs_ref, mine_ref)):

        @pl.when(at_ref[0] == k)
        def _():
            out_ref[:, :, :outs] = first[...]
            out_ref[:, :, outs:] = second[...]


def grant(mebibytes):
    return pltpu.CompilerParams(vmem_limit_bytes=mebibytes << 20)


VM = pl.BlockSpec(memory_space=pltpu.VMEM)
SM = pl.BlockSpec(memory_space=pltpu.SMEM)
HB = pl.BlockSpec(memory_space=pltpu.HBM)


def on_device(
    features,
    first_gain,
    first_shift,
    first_weight,
    first_bias,
    second_gain,
    second_shift,
    second_weight,
    second_bias,
    upsample_weight,
    upsample_bias,
):
    _, breadth, channels = features.shape
    nx, nzh, nzl, ncol = (lax.axis_size(axis) for axis in ("x", "zh", "zl", "col"))
    nz = nzh * nzl
    k_own = first_weight.shape[2]
    cols = breadth * ncol
    half = channels // ncol
    depth = channels // nzl
    image_rows = nx * nz
    per_group = channels // G
    count = image_rows * cols * per_group
    c = lax.axis_index("col")
    zl = lax.axis_index("zl")
    at = lax.axis_index(ROW).astype(jnp.int32)[None]

    def order(v, axes):
        v = v.reshape(-1, nx, nzh, nzl, k_own).transpose(0, *[k + 1 for k in axes], 4)
        return v.reshape(-1, channels)

    place = lax.broadcasted_iota(jnp.int32, (channels, channels), 1)
    natural = lax.broadcasted_iota(jnp.int32, (channels, channels), 0)
    k, x = place % k_own, place // k_own % nx
    line = place // (k_own * nx)
    source = (x * nz + line) * k_own + k
    move = (natural == source).astype(BF16)
    source = (x * nz + line % nzh * nzl + line // nzh) * k_own + k
    move_one = (natural == source).astype(BF16)

    def moved(v, by):
        return jnp.dot(v, by, preferred_element_type=F32).astype(BF16)

    def own_half(v):
        return lax.dynamic_slice_in_dim(v, c * half, half, v.ndim - 1)

    taps = 9 * k_own
    hold = moved(
        jnp.concatenate([first_weight.reshape(taps, channels), second_weight.reshape(taps, channels)]),
        move,
    )
    hold = jnp.concatenate([hold, upsample_weight.reshape(taps, channels)])
    hold = own_half(hold).reshape(1, 27, k_own, half)
    hold = lax.all_to_all(jnp.broadcast_to(hold, (nx, 27, k_own, half)), "x", 0, 0, tiled=True)
    hold = hold.transpose(1, 0, 2, 3).reshape(27, nx * k_own, half)
    weights = lax.all_gather(hold[9:], ("zh", "zl"))
    hold_one = hold[:9]

    own = features[0]
    wide = own.astype(F32)
    chan = lax.broadcasted_iota(jnp.int32, (channels, G), 0) // per_group
    member = (chan == lax.broadcasted_iota(jnp.int32, (channels, G), 1)).astype(F32)
    sums = jnp.stack([jnp.sum(wide, axis=0), jnp.sum(wide * wide, axis=0)])
    sums = jnp.dot(sums, member, precision=HIGHEST).reshape(1, 2 * G)
    sums = jnp.pad(sums, ((0, 0), (0, 128 - 2 * G)))
    sums = jnp.sum(sum_over(sums, ("x", "zl", "col")), axis=0, keepdims=True)
    high = lax.reduce_precision(sums, 8, 7)
    low = lax.reduce_precision(sums - high, 8, 7)
    terms = jnp.concatenate([high, low, sums - high - low]).astype(BF16)
    terms = jnp.pad(terms, ((0, nx * k_own - 3), (0, half - 128)))
    weights_one = lax.all_gather(jnp.concatenate([hold_one, terms[None]]), "zh")

    last = nx * nz - 1
    pairs = [(i, i + 1) for i in range(nzl - 1, last, nzl)] + [(i, i - 1) for i in range(nzl, last, nzl)]
    edge = lax.ppermute(own, ROW, pairs)
    sent = moved(jnp.concatenate([own, edge]), move_one)
    sent = sent.reshape(2, breadth, nzl, depth).transpose(2, 0, 1, 3)
    sent = jnp.broadcast_to(sent[:, None], (nzl, ncol, 2, breadth, depth))
    sent = sent.reshape(nzl * ncol, 2, breadth, depth)
    quad = lax.all_to_all(sent, ("zl", "col"), 0, 0, tiled=True)

    quad = quad.reshape(nzl, ncol, 2, breadth, depth)

    def own_depth(v):
        return lax.dynamic_slice_in_dim(v, zl * depth, depth, 1)

    gain_one = own_depth(order(first_gain, (2, 1, 0)))
    shift_one = own_depth(order(first_shift, (2, 1, 0)))
    vectors = order(jnp.stack([second_gain, second_shift, first_bias, second_bias]), (1, 2, 0))
    gain_two, shift_two = vectors[:1], vectors[1:2]
    vectors = own_half(jnp.concatenate([vectors[2:], upsample_bias[None]]))
    bias_one, bias_two, bias_up = [vectors[i : i + 1] for i in range(3)]

    def picks(group, groups):
        pick = group[:, None] == jnp.arange(128)[None, :]
        return jnp.concatenate([pick, jnp.roll(pick, groups, axis=1)]).astype(F32)

    lane = jnp.arange(depth)
    pick_one = picks(lane // k_own % nx * nzh + lane // (k_own * nx), G)
    lane = jnp.arange(channels)
    group = lane // (k_own * nx * nzl) * nx + lane // k_own % nx
    pick_two = picks(group, G)
    pick_own = picks(group[:half] + c * (G // ncol), G)

    parts = pl.pallas_call(
        functools.partial(conv_one_kernel, cols, image_rows, count),
        out_shape=jax.ShapeDtypeStruct((nzl, cols, half), BF16),
        in_specs=[SM] + [VM] * 5,
        out_specs=VM,
        scratch_shapes=[pltpu.VMEM(((nzl + 2) * cols, 3 * depth), BF16)],
        compiler_params=grant(16),
        name="conv_one",
    )(at, quad, gain_one, shift_one, pick_one, weights_one)
    parts, own = lax.optimization_barrier((parts, own))
    parts = lax.all_to_all(parts, "zl", 0, 0, tiled=True)
    three = [shifted_rows(own, ROW, -1), own, shifted_rows(own, ROW, 1)]
    hidden, sums_two = pl.pallas_call(
        join_kernel,
        out_shape=(
            jax.ShapeDtypeStruct((cols, half), BF16),
            jax.ShapeDtypeStruct((8, 128), F32),
        ),
        in_specs=[VM] * 3,
        out_specs=(VM, VM),
        compiler_params=grant(8),
        name="join_one",
    )(parts, bias_one, pick_own)

    both = lax.all_gather(hidden, "col")
    three, _ = lax.optimization_barrier((three, sums_two))
    stats = jnp.sum(sum_over(sums_two[:1], ("x", "zl", "col")), axis=0, keepdims=True)
    three = lax.all_gather(jnp.stack(three), "col", axis=1, tiled=True)
    residual = own_half(moved(three.reshape(3 * cols, channels), move))
    stats, both, residual = lax.optimization_barrier((stats, both, residual))
    stats = sum_over(stats, "zh")
    far = jnp.stack([lax.ppermute(both, ROW + ("col",), fetch(nx * nz, d)) for d in (1, 2)])
    far = lax.all_gather(far, "col")
    normed = pl.pallas_call(
        functools.partial(norm_kernel, image_rows, count),
        out_shape=jax.ShapeDtypeStruct((ncol, 5 * cols, half), BF16),
        in_specs=[SM] + [VM] * 6,
        out_specs=VM,
        compiler_params=grant(12),
        name="norm_two",
    )(at, both, far, stats, gain_two, shift_two, pick_two)

    rows = 3
    held = [
        pltpu.VMEM((9, weights.shape[0]) + weights.shape[2:], BF16),
        pltpu.SemaphoreType.DMA((9,)),
    ]
    block = pl.pallas_call(
        functools.partial(conv_two_kernel, cols, rows, image_rows),
        out_shape=jax.ShapeDtypeStruct((rows * cols, half), BF16),
        in_specs=[SM, VM, VM, VM, HB],
        out_specs=VM,
        scratch_shapes=[pltpu.VMEM((3, (rows + 2) * cols, channels), BF16)] + held,
        compiler_params=grant(58),
        name="conv_two",
    )(at, normed, residual, bias_two, weights)
    block = lax.all_gather(block, "col")

    core = c.astype(jnp.int32)[None]
    side = jax.ShapeDtypeStruct((2, cols, half), BF16)
    mine, theirs = pl.pallas_call(
        functools.partial(conv_up_kernel, cols),
        out_shape=(side, side),
        in_specs=[SM, VM, VM, HB],
        out_specs=(VM, VM),
        scratch_shapes=[
            pltpu.VMEM((3, 3 * cols, channels), BF16),
            pltpu.VMEM((2, 2, 2 * cols, 128), F32),
        ]
        + held,
        compiler_params=grant(58),
        name="conv_up",
    )(core, block, bias_up, weights)
    theirs = lax.ppermute(theirs, "col", [(0, 1), (1, 0)])
    return pl.pallas_call(
        sides_kernel,
        out_shape=jax.ShapeDtypeStruct((2, cols, channels), BF16),
        in_specs=[SM, VM, VM],
        out_specs=VM,
        compiler_params=grant(8),
        name="sides",
    )(core, mine, theirs)


def solution(mesh):
    finer = Mesh(
        mesh.devices.reshape(mesh.shape["img"], 4, 8, 4, mesh.shape["col"]),
        IMG_ROW + ("col",),
    )
    in_specs = (
        P(IMG_ROW, "col", None),
        P(),
        P(),
        P(None, None, ROW, None),
        P(),
        P(),
        P(),
        P(None, None, ROW, None),
        P(),
        P(None, None, ROW, None),
        P(),
    )

    return jax.shard_map(
        on_device,
        mesh=finer,
        in_specs=in_specs,
        out_specs=P(IMG_ROW, "col", None),
        check_vma=False,
    )
```

```python
import functools

import jax
import jax.numpy as jnp
from jax import lax
from jax.experimental import pallas as pl
from jax.experimental.pallas import tpu as pltpu
from jax.sharding import Mesh
from jax.sharding import PartitionSpec as P

G = 32
EPS = 1e-06
F32, BF16 = jnp.float32, jnp.bfloat16
HIGHEST = lax.Precision.HIGHEST
ROW = ("x", "zh", "zl")
IMG_ROW = ("img",) + ROW


def sum_over(vector, axes):
    count = lax.axis_size(axes)
    sent = jnp.broadcast_to(vector, (count, vector.shape[1]))
    return lax.all_to_all(sent, axes, 0, 0, tiled=True)


def shifted_rows(values, axis, by):
    count = lax.axis_size(axis)
    pairs = [(i, i - by) for i in range(count) if 0 <= i - by < count]
    return lax.ppermute(values, axis, pairs)


def fetch(count, by):
    above = [(2 * (i - by), 2 * i) for i in range(by, count)]
    return above + [(2 * (i + by) + 1, 2 * i + 1) for i in range(count - by)]


def silu(u):
    return u / (1.0 + jnp.exp(-u))


def spread_stats(totals, pick, count, gain, shift):
    totals = jnp.broadcast_to(totals, (8, totals.shape[1]))
    spread = lax.dot_general(
        totals, pick, (((1,), (1,)), ((), ())), precision=HIGHEST, preferred_element_type=F32
    )
    width = gain.shape[1]
    mean = spread[:1, :width] / count
    var = spread[:1, width:] / count - mean * mean
    a = lax.rsqrt(var + EPS) * gain
    return a, shift - mean * a


def conv_one_kernel(cols, image_rows, count, at_ref, x_ref, gain_ref, shift_ref, pick_ref, w_ref, out_ref, S):
    quad, depth = x_ref.shape[0], x_ref.shape[4]
    totals = jnp.sum(w_ref[:, 9, :, :128].astype(F32).reshape(-1, 128), axis=0, keepdims=True)
    a, b = spread_stats(totals, pick_ref[...], count, gain_ref[...], shift_ref[...])
    first = at_ref[0] // quad * quad - 1
    column = lax.broadcasted_iota(jnp.int32, (cols, depth), 0)
    for i in range(quad + 2):
        member = min(max(i - 1, 0), quad - 1)
        slot = 0 if 1 <= i <= quad else 1
        x = jnp.concatenate([x_ref[member, h, slot] for h in range(x_ref.shape[1])], axis=0)
        y = silu(x.astype(F32) * a + b)
        if slot:
            y = jnp.where(jnp.logical_and(first + i >= 0, first + i < image_rows), y, 0.0)
        at = slice(i * cols, (i + 1) * cols)
        left = jnp.where(column == 0, 0.0, pltpu.roll(y, 1, 0))
        right = jnp.where(column == cols - 1, 0.0, pltpu.roll(y, cols - 1, 0))
        S[at, 0 * depth : 1 * depth] = left.astype(BF16)
        S[at, 1 * depth : 2 * depth] = y.astype(BF16)
        S[at, 2 * depth : 3 * depth] = right.astype(BF16)
    outs = out_ref.shape[2]
    total = jnp.zeros((quad * cols, outs), F32)
    for r in range(3):
        piece = jnp.concatenate([w_ref[:, 3 * r + k].reshape(depth, outs) for k in range(3)], axis=0)
        total += jnp.dot(S[r * cols : (r + quad) * cols, :], piece, preferred_element_type=F32)
    out_ref[...] = total.astype(BF16).reshape(quad, cols, outs)


def join_kernel(x_ref, bias_ref, pick_ref, out_ref, sums_ref):
    total = x_ref[0].astype(F32)
    for k in range(1, x_ref.shape[0]):
        total += x_ref[k].astype(F32)
    hidden = (total + bias_ref[...]).astype(BF16)
    out_ref[...] = hidden
    own = hidden.astype(F32)
    both = jnp.concatenate(
        [jnp.sum(own, axis=0, keepdims=True), jnp.sum(own * own, axis=0, keepdims=True)], axis=1
    )
    both = jnp.broadcast_to(both, (8, both.shape[1]))
    sums_ref[...] = jnp.dot(both, pick_ref[...], precision=HIGHEST, preferred_element_type=F32)


def norm_kernel(image_rows, count, at_ref, own_ref, far_ref, stats_ref, gain_ref, shift_ref, pick_ref, out_ref):
    totals = jnp.sum(stats_ref[...], axis=0, keepdims=True)
    a, b = spread_stats(totals, pick_ref[...], count, gain_ref[...], shift_ref[...])
    halves, cols, half = own_ref.shape
    for d in range(-2, 3):
        row = at_ref[0] + d
        inside = jnp.logical_and(row >= 0, row < image_rows)
        for h in range(halves):
            lanes = slice(h * half, (h + 1) * half)
            x = far_ref[int(d > 0), abs(d) - 1, h] if d else own_ref[h]
            y = silu(x.astype(F32) * a[:, lanes] + b[:, lanes])
            out_ref[h, (d + 2) * cols : (d + 3) * cols, :] = jnp.where(inside, y, 0.0).astype(BF16)


def fetch_weights(w_ref, base, held, arrived):
    lines = held.shape[1]
    copies = [
        pltpu.make_async_copy(
            w_ref.at[pl.ds(h * lines, lines), pl.ds(base, 9)], held.at[h], arrived.at[h]
        )
        for h in range(2)
    ]
    for copy in copies:
        copy.start()
    return copies


def moved_right(y, cols):
    column = lax.broadcasted_iota(jnp.int32, y.shape, 0) % cols
    return jnp.where(column == 0, 0.0, pltpu.roll(y, 1, 0))


def moved_left(y, cols):
    column = lax.broadcasted_iota(jnp.int32, y.shape, 0) % cols
    return jnp.where(column == cols - 1, 0.0, pltpu.roll(y, y.shape[0] - 1, 0))


def conv_two_kernel(cols, rows, image_rows, at_ref, x_ref, res_ref, bias_ref, w_ref, out_ref, held, arrived):
    copies = fetch_weights(w_ref, 0, held, arrived)
    outs = out_ref.shape[1]
    totals = [jnp.zeros(out_ref.shape, F32) for _ in range(3)]
    for h in range(2):
        copies[h].wait()
        for r in range(3):
            x = x_ref[h, r * cols : (r + rows) * cols, :]
            for k in range(3):
                piece = held[h, :, 3 * r + k].reshape(-1, outs)
                totals[k] += jnp.dot(x, piece, preferred_element_type=F32)
    total = totals[1] + moved_right(totals[0], cols) + moved_left(totals[2], cols) + bias_ref[...]
    first = at_ref[0] - rows // 2
    for i in range(rows):
        at = slice(i * cols, (i + 1) * cols)
        y = total[at] + res_ref[at, :].astype(F32)
        inside = jnp.logical_and(first + i >= 0, first + i < image_rows)
        out_ref[at, :] = jnp.where(inside, y, 0.0).astype(BF16)


def conv_up_kernel(cols, at_ref, x_ref, bias_ref, w_ref, mine_ref, theirs_ref, full, held, arrived):
    copies = fetch_weights(w_ref, 9, held, arrived)
    outs = mine_ref.shape[2]
    totals = [jnp.zeros((2 * cols, outs), F32) for _ in range(3)]
    for h in range(2):
        copies[h].wait()
        for r in range(3):
            starts = [(r + 1 + p) // 2 * cols for p in range(2)]
            x = jnp.concatenate([x_ref[h, start : start + cols, :] for start in starts])
            for k in range(3):
                piece = held[h, :, 3 * r + k].reshape(-1, outs)
                totals[k] += jnp.dot(x, piece, preferred_element_type=F32)
    middle = totals[1] + bias_ref[...]
    even = moved_right(totals[0], cols) + middle + totals[2]
    odd = totals[0] + middle + moved_left(totals[2], cols)
    mine = pl.multiple_of(at_ref[0] * cols, cols)
    theirs = pl.multiple_of((1 - at_ref[0]) * cols, cols)
    for p in range(2):
        for k in range(2):
            lanes = slice(k * 128, (k + 1) * 128)
            for q, y in enumerate((even, odd)):
                full[p, k, pl.ds(q, cols, stride=2), :] = y[p * cols : (p + 1) * cols, lanes]
            mine_ref[p, :, lanes] = full[p, k, pl.ds(mine, cols), :].astype(BF16)
            theirs_ref[p, :, lanes] = full[p, k, pl.ds(theirs, cols), :].astype(BF16)


def sides_kernel(at_ref, mine_ref, theirs_ref, out_ref):
    outs = mine_ref.shape[2]
    for k, first, second in ((0, mine_ref, theirs_ref), (1, theirs_ref, mine_ref)):

        @pl.when(at_ref[0] == k)
        def _():
            out_ref[:, :, :outs] = first[...]
            out_ref[:, :, outs:] = second[...]


def grant(mebibytes):
    return pltpu.CompilerParams(vmem_limit_bytes=mebibytes << 20)


VM = pl.BlockSpec(memory_space=pltpu.VMEM)
SM = pl.BlockSpec(memory_space=pltpu.SMEM)
HB = pl.BlockSpec(memory_space=pltpu.HBM)


def on_device(
    features,
    first_gain,
    first_shift,
    first_weight,
    first_bias,
    second_gain,
    second_shift,
    second_weight,
    second_bias,
    upsample_weight,
    upsample_bias,
):
    _, breadth, channels = features.shape
    nx, nzh, nzl, ncol = (lax.axis_size(axis) for axis in ("x", "zh", "zl", "col"))
    nz = nzh * nzl
    k_own = first_weight.shape[2]
    cols = breadth * ncol
    half = channels // ncol
    depth = channels // nzl
    image_rows = nx * nz
    per_group = channels // G
    count = image_rows * cols * per_group
    c = lax.axis_index("col")
    zl = lax.axis_index("zl")
    at = lax.axis_index(ROW).astype(jnp.int32)[None]

    def order(v, axes):
        v = v.reshape(-1, nx, nzh, nzl, k_own).transpose(0, *[k + 1 for k in axes], 4)
        return v.reshape(-1, channels)

    place = lax.broadcasted_iota(jnp.int32, (channels, channels), 1)
    natural = lax.broadcasted_iota(jnp.int32, (channels, channels), 0)
    k, x = place % k_own, place // k_own % nx
    line = place // (k_own * nx)
    source = (x * nz + line) * k_own + k
    move = (natural == source).astype(BF16)
    source = (x * nz + line % nzh * nzl + line // nzh) * k_own + k
    move_one = (natural == source).astype(BF16)

    def moved(v, by):
        return jnp.dot(v, by, preferred_element_type=F32).astype(BF16)

    def own_half(v):
        return lax.dynamic_slice_in_dim(v, c * half, half, v.ndim - 1)

    taps = 9 * k_own
    hold = moved(
        jnp.concatenate([first_weight.reshape(taps, channels), second_weight.reshape(taps, channels)]),
        move,
    )
    hold = jnp.concatenate([hold, upsample_weight.reshape(taps, channels)])
    hold = own_half(hold).reshape(1, 27, k_own, half)
    hold = lax.all_to_all(jnp.broadcast_to(hold, (nx, 27, k_own, half)), "x", 0, 0, tiled=True)
    hold = hold.transpose(1, 0, 2, 3).reshape(27, nx * k_own, half)
    weights = lax.all_gather(hold[9:], ("zh", "zl"))
    hold_one = hold[:9]

    own = features[0]
    wide = own.astype(F32)
    chan = lax.broadcasted_iota(jnp.int32, (channels, G), 0) // per_group
    member = (chan == lax.broadcasted_iota(jnp.int32, (channels, G), 1)).astype(F32)
    sums = jnp.stack([jnp.sum(wide, axis=0), jnp.sum(wide * wide, axis=0)])
    sums = jnp.dot(sums, member, precision=HIGHEST).reshape(1, 2 * G)
    sums = jnp.pad(sums, ((0, 0), (0, 128 - 2 * G)))
    sums = jnp.sum(sum_over(sums, ("x", "zl", "col")), axis=0, keepdims=True)
    high = lax.reduce_precision(sums, 8, 7)
    low = lax.reduce_precision(sums - high, 8, 7)
    terms = jnp.concatenate([high, low, sums - high - low]).astype(BF16)
    terms = jnp.pad(terms, ((0, nx * k_own - 3), (0, half - 128)))
    weights_one = lax.all_gather(jnp.concatenate([hold_one, terms[None]]), "zh")

    last = nx * nz - 1
    pairs = [(i, i + 1) for i in range(nzl - 1, last, nzl)] + [(i, i - 1) for i in range(nzl, last, nzl)]
    edge = lax.ppermute(own, ROW, pairs)
    sent = moved(jnp.concatenate([own, edge]), move_one)
    sent = sent.reshape(2, breadth, nzl, depth).transpose(2, 0, 1, 3)
    sent = jnp.broadcast_to(sent[:, None], (nzl, ncol, 2, breadth, depth))
    sent = sent.reshape(nzl * ncol, 2, breadth, depth)
    quad = lax.all_to_all(sent, ("zl", "col"), 0, 0, tiled=True)

    quad = quad.reshape(nzl, ncol, 2, breadth, depth)

    def own_depth(v):
        return lax.dynamic_slice_in_dim(v, zl * depth, depth, 1)

    gain_one = own_depth(order(first_gain, (2, 1, 0)))
    shift_one = own_depth(order(first_shift, (2, 1, 0)))
    vectors = order(jnp.stack([second_gain, second_shift, first_bias, second_bias]), (1, 2, 0))
    gain_two, shift_two = vectors[:1], vectors[1:2]
    vectors = own_half(jnp.concatenate([vectors[2:], upsample_bias[None]]))
    bias_one, bias_two, bias_up = [vectors[i : i + 1] for i in range(3)]

    def picks(group, groups):
        pick = group[:, None] == jnp.arange(128)[None, :]
        return jnp.concatenate([pick, jnp.roll(pick, groups, axis=1)]).astype(F32)

    lane = jnp.arange(depth)
    pick_one = picks(lane // k_own % nx * nzh + lane // (k_own * nx), G)
    lane = jnp.arange(channels)
    group = lane // (k_own * nx * nzl) * nx + lane // k_own % nx
    pick_two = picks(group, G)
    pick_own = picks(group[:half] + c * (G // ncol), G)

    parts = pl.pallas_call(
        functools.partial(conv_one_kernel, cols, image_rows, count),
        out_shape=jax.ShapeDtypeStruct((nzl, cols, half), BF16),
        in_specs=[SM] + [VM] * 5,
        out_specs=VM,
        scratch_shapes=[pltpu.VMEM(((nzl + 2) * cols, 3 * depth), BF16)],
        compiler_params=grant(16),
        name="conv_one",
    )(at, quad, gain_one, shift_one, pick_one, weights_one)
    parts, own = lax.optimization_barrier((parts, own))
    parts = lax.all_to_all(parts, "zl", 0, 0, tiled=True)
    three = [shifted_rows(own, ROW, -1), own, shifted_rows(own, ROW, 1)]
    hidden, sums_two = pl.pallas_call(
        join_kernel,
        out_shape=(
            jax.ShapeDtypeStruct((cols, half), BF16),
            jax.ShapeDtypeStruct((8, 128), F32),
        ),
        in_specs=[VM] * 3,
        out_specs=(VM, VM),
        compiler_params=grant(8),
        name="join_one",
    )(parts, bias_one, pick_own)

    both = lax.all_gather(hidden, "col")
    three, _ = lax.optimization_barrier((three, sums_two))
    stats = sum_over(sums_two[:1], ("x", "zl", "col"))
    stats = jnp.sum(stats, axis=0, keepdims=True)
    three = lax.all_gather(jnp.stack(three), "col", axis=1, tiled=True)
    residual = own_half(moved(three.reshape(3 * cols, channels), move))
    stats, both, residual = lax.optimization_barrier((stats, both, residual))
    stats = sum_over(stats, "zh")
    far = jnp.stack([lax.ppermute(both, ROW + ("col",), fetch(nx * nz, d)) for d in (1, 2)])
    far = lax.all_gather(far, "col")
    normed = pl.pallas_call(
        functools.partial(norm_kernel, image_rows, count),
        out_shape=jax.ShapeDtypeStruct((ncol, 5 * cols, half), BF16),
        in_specs=[SM] + [VM] * 6,
        out_specs=VM,
        compiler_params=grant(12),
        name="norm_two",
    )(at, both, far, stats, gain_two, shift_two, pick_two)

    rows = 3
    held = [
        pltpu.VMEM((2, nz // 2, 9) + weights.shape[2:], BF16),
        pltpu.SemaphoreType.DMA((2,)),
    ]
    block = pl.pallas_call(
        functools.partial(conv_two_kernel, cols, rows, image_rows),
        out_shape=jax.ShapeDtypeStruct((rows * cols, half), BF16),
        in_specs=[SM, VM, VM, VM, HB],
        out_specs=VM,
        scratch_shapes=held,
        compiler_params=grant(50),
        name="conv_two",
    )(at, normed, residual, bias_two, weights)
    block = lax.all_gather(block, "col")

    core = c.astype(jnp.int32)[None]
    side = jax.ShapeDtypeStruct((2, cols, half), BF16)
    mine, theirs = pl.pallas_call(
        functools.partial(conv_up_kernel, cols),
        out_shape=(side, side),
        in_specs=[SM, VM, VM, HB],
        out_specs=(VM, VM),
        scratch_shapes=[pltpu.VMEM((2, 2, 2 * cols, 128), F32)] + held,
        compiler_params=grant(50),
        name="conv_up",
    )(core, block, bias_up, weights)
    theirs = lax.ppermute(theirs, "col", [(0, 1), (1, 0)])
    return pl.pallas_call(
        sides_kernel,
        out_shape=jax.ShapeDtypeStruct((2, cols, channels), BF16),
        in_specs=[SM, VM, VM],
        out_specs=VM,
        compiler_params=grant(8),
        name="sides",
    )(core, mine, theirs)


def solution(mesh):
    finer = Mesh(
        mesh.devices.reshape(mesh.shape["img"], 4, 8, 4, mesh.shape["col"]),
        IMG_ROW + ("col",),
    )
    in_specs = (
        P(IMG_ROW, "col", None),
        P(),
        P(),
        P(None, None, ROW, None),
        P(),
        P(),
        P(),
        P(None, None, ROW, None),
        P(),
        P(None, None, ROW, None),
        P(),
    )

    return jax.shard_map(
        on_device,
        mesh=finer,
        in_specs=in_specs,
        out_specs=P(IMG_ROW, "col", None),
        check_vma=False,
    )
```

```python
import functools

import jax
import jax.numpy as jnp
from jax import lax
from jax.experimental import pallas as pl
from jax.experimental.pallas import tpu as pltpu
from jax.sharding import Mesh
from jax.sharding import PartitionSpec as P

G = 32
EPS = 1e-06
F32, BF16 = jnp.float32, jnp.bfloat16
HIGHEST = lax.Precision.HIGHEST
ROW = ("x", "zh", "zl")
IMG_ROW = ("img",) + ROW


def sum_over(vector, axes):
    count = lax.axis_size(axes)
    sent = jnp.broadcast_to(vector, (count, vector.shape[1]))
    return lax.all_to_all(sent, axes, 0, 0, tiled=True)


def shifted_rows(values, axis, by):
    count = lax.axis_size(axis)
    pairs = [(i, i - by) for i in range(count) if 0 <= i - by < count]
    return lax.ppermute(values, axis, pairs)


def fetch(count, by):
    above = [(2 * (i - by), 2 * i) for i in range(by, count)]
    return above + [(2 * (i + by) + 1, 2 * i + 1) for i in range(count - by)]


def silu(u):
    return u / (1.0 + jnp.exp(-u))


def prep_kernel(nx, k_own, core_ref, one_ref, two_ref, up_ref, out_ref):
    taps, _, channels = one_ref.shape
    half = out_ref.shape[3]
    place = lax.broadcasted_iota(jnp.int32, (channels, half), 1) + core_ref[0] * half
    natural = lax.broadcasted_iota(jnp.int32, (channels, half), 0)
    line, x, k = place // (k_own * nx), place // k_own % nx, place % k_own
    move = (natural == (x * (channels // (nx * k_own)) + line) * k_own + k).astype(BF16)
    rows = [ref[t].astype(F32) for ref in (one_ref, two_ref) for t in range(taps)]
    moved = jnp.dot(jnp.concatenate(rows).astype(BF16), move, preferred_element_type=F32)
    lanes = pl.ds(pl.multiple_of(core_ref[0] * half, half), half)
    for d in range(nx):
        for t in range(2 * taps):
            out_ref[d, t] = moved[t * k_own : (t + 1) * k_own].astype(BF16)
        out_ref[d, 2 * taps :] = up_ref[:, :, lanes]


def spread_stats(totals, pick, count, gain, shift):
    totals = jnp.broadcast_to(totals, (8, totals.shape[1]))
    spread = lax.dot_general(
        totals, pick, (((1,), (1,)), ((), ())), precision=HIGHEST, preferred_element_type=F32
    )
    width = gain.shape[1]
    mean = spread[:1, :width] / count
    var = spread[:1, width:] / count - mean * mean
    a = lax.rsqrt(var + EPS) * gain
    return a, shift - mean * a


def conv_one_kernel(cols, image_rows, count, at_ref, x_ref, gain_ref, shift_ref, pick_ref, w_ref, out_ref, S):
    quad, depth = x_ref.shape[0], x_ref.shape[4]
    totals = jnp.sum(w_ref[:, 9, :, :128].astype(F32).reshape(-1, 128), axis=0, keepdims=True)
    a, b = spread_stats(totals, pick_ref[...], count, gain_ref[...], shift_ref[...])
    first = at_ref[0] // quad * quad - 1
    column = lax.broadcasted_iota(jnp.int32, (cols, depth), 0)
    for i in range(quad + 2):
        member = min(max(i - 1, 0), quad - 1)
        slot = 0 if 1 <= i <= quad else 1
        x = jnp.concatenate([x_ref[member, h, slot] for h in range(x_ref.shape[1])], axis=0)
        y = silu(x.astype(F32) * a + b)
        if slot:
            y = jnp.where(jnp.logical_and(first + i >= 0, first + i < image_rows), y, 0.0)
        at = slice(i * cols, (i + 1) * cols)
        left = jnp.where(column == 0, 0.0, pltpu.roll(y, 1, 0))
        right = jnp.where(column == cols - 1, 0.0, pltpu.roll(y, cols - 1, 0))
        S[at, 0 * depth : 1 * depth] = left.astype(BF16)
        S[at, 1 * depth : 2 * depth] = y.astype(BF16)
        S[at, 2 * depth : 3 * depth] = right.astype(BF16)
    outs = out_ref.shape[2]
    total = jnp.zeros((quad * cols, outs), F32)
    for r in range(3):
        piece = jnp.concatenate([w_ref[:, 3 * r + k].reshape(depth, outs) for k in range(3)], axis=0)
        total += jnp.dot(S[r * cols : (r + quad) * cols, :], piece, preferred_element_type=F32)
    out_ref[...] = total.astype(BF16).reshape(quad, cols, outs)


def join_kernel(x_ref, bias_ref, pick_ref, out_ref, sums_ref):
    total = x_ref[0].astype(F32)
    for k in range(1, x_ref.shape[0]):
        total += x_ref[k].astype(F32)
    hidden = (total + bias_ref[...]).astype(BF16)
    out_ref[...] = hidden
    own = hidden.astype(F32)
    both = jnp.concatenate(
        [jnp.sum(own, axis=0, keepdims=True), jnp.sum(own * own, axis=0, keepdims=True)], axis=1
    )
    both = jnp.broadcast_to(both, (8, both.shape[1]))
    sums_ref[...] = jnp.dot(both, pick_ref[...], precision=HIGHEST, preferred_element_type=F32)


def norm_kernel(image_rows, count, at_ref, own_ref, far_ref, stats_ref, gain_ref, shift_ref, pick_ref, out_ref):
    totals = jnp.sum(stats_ref[...], axis=0, keepdims=True)
    a, b = spread_stats(totals, pick_ref[...], count, gain_ref[...], shift_ref[...])
    halves, cols, half = own_ref.shape
    for d in range(-2, 3):
        row = at_ref[0] + d
        inside = jnp.logical_and(row >= 0, row < image_rows)
        for h in range(halves):
            lanes = slice(h * half, (h + 1) * half)
            x = far_ref[int(d > 0), abs(d) - 1, h] if d else own_ref[h]
            y = silu(x.astype(F32) * a[:, lanes] + b[:, lanes])
            out_ref[h, (d + 2) * cols : (d + 3) * cols, :] = jnp.where(inside, y, 0.0).astype(BF16)


def fetch_weights(w_ref, base, held, arrived):
    lines = held.shape[1]
    copies = [
        pltpu.make_async_copy(
            w_ref.at[pl.ds(h * lines, lines), pl.ds(base, 9)], held.at[h], arrived.at[h]
        )
        for h in range(2)
    ]
    for copy in copies:
        copy.start()
    return copies


def moved_right(y, cols):
    column = lax.broadcasted_iota(jnp.int32, y.shape, 0) % cols
    return jnp.where(column == 0, 0.0, pltpu.roll(y, 1, 0))


def moved_left(y, cols):
    column = lax.broadcasted_iota(jnp.int32, y.shape, 0) % cols
    return jnp.where(column == cols - 1, 0.0, pltpu.roll(y, y.shape[0] - 1, 0))


def conv_two_kernel(cols, rows, image_rows, at_ref, x_ref, res_ref, bias_ref, w_ref, out_ref, held, arrived):
    copies = fetch_weights(w_ref, 0, held, arrived)
    outs = out_ref.shape[1]
    totals = [jnp.zeros(out_ref.shape, F32) for _ in range(3)]
    for h in range(2):
        copies[h].wait()
        for r in range(3):
            x = x_ref[h, r * cols : (r + rows) * cols, :]
            for k in range(3):
                piece = held[h, :, 3 * r + k].reshape(-1, outs)
                totals[k] += jnp.dot(x, piece, preferred_element_type=F32)
    total = totals[1] + moved_right(totals[0], cols) + moved_left(totals[2], cols) + bias_ref[...]
    first = at_ref[0] - rows // 2
    for i in range(rows):
        at = slice(i * cols, (i + 1) * cols)
        y = total[at] + res_ref[at, :].astype(F32)
        inside = jnp.logical_and(first + i >= 0, first + i < image_rows)
        out_ref[at, :] = jnp.where(inside, y, 0.0).astype(BF16)


def conv_up_kernel(cols, at_ref, x_ref, bias_ref, w_ref, mine_ref, theirs_ref, full):
    lines = w_ref.shape[0] // 2
    outs = mine_ref.shape[2]
    totals = [jnp.zeros((2 * cols, outs), F32) for _ in range(3)]
    for h in range(2):
        for r in range(3):
            starts = [(r + 1 + p) // 2 * cols for p in range(2)]
            x = jnp.concatenate([x_ref[h, start : start + cols, :] for start in starts])
            for k in range(3):
                piece = w_ref[h * lines : (h + 1) * lines, 9 + 3 * r + k].reshape(-1, outs)
                totals[k] += jnp.dot(x, piece, preferred_element_type=F32)
    middle = totals[1] + bias_ref[...]
    even = moved_right(totals[0], cols) + middle + totals[2]
    odd = totals[0] + middle + moved_left(totals[2], cols)
    mine = pl.multiple_of(at_ref[0] * cols, cols)
    theirs = pl.multiple_of((1 - at_ref[0]) * cols, cols)
    for p in range(2):
        for k in range(2):
            lanes = slice(k * 128, (k + 1) * 128)
            for q, y in enumerate((even, odd)):
                full[p, k, pl.ds(q, cols, stride=2), :] = y[p * cols : (p + 1) * cols, lanes]
            mine_ref[p, :, lanes] = full[p, k, pl.ds(mine, cols), :].astype(BF16)
            theirs_ref[p, :, lanes] = full[p, k, pl.ds(theirs, cols), :].astype(BF16)


def sides_kernel(at_ref, mine_ref, theirs_ref, out_ref):
    outs = mine_ref.shape[2]
    for k, first, second in ((0, mine_ref, theirs_ref), (1, theirs_ref, mine_ref)):

        @pl.when(at_ref[0] == k)
        def _():
            out_ref[:, :, :outs] = first[...]
            out_ref[:, :, outs:] = second[...]


def grant(mebibytes):
    return pltpu.CompilerParams(vmem_limit_bytes=mebibytes << 20)


VM = pl.BlockSpec(memory_space=pltpu.VMEM)
SM = pl.BlockSpec(memory_space=pltpu.SMEM)
HB = pl.BlockSpec(memory_space=pltpu.HBM)


def on_device(
    features,
    first_gain,
    first_shift,
    first_weight,
    first_bias,
    second_gain,
    second_shift,
    second_weight,
    second_bias,
    upsample_weight,
    upsample_bias,
):
    _, breadth, channels = features.shape
    nx, nzh, nzl, ncol = (lax.axis_size(axis) for axis in ("x", "zh", "zl", "col"))
    nz = nzh * nzl
    k_own = first_weight.shape[2]
    cols = breadth * ncol
    half = channels // ncol
    depth = channels // nzl
    image_rows = nx * nz
    per_group = channels // G
    count = image_rows * cols * per_group
    c = lax.axis_index("col")
    zl = lax.axis_index("zl")
    at = lax.axis_index(ROW).astype(jnp.int32)[None]

    def order(v, axes):
        v = v.reshape(-1, nx, nzh, nzl, k_own).transpose(0, *[k + 1 for k in axes], 4)
        return v.reshape(-1, channels)

    place = lax.broadcasted_iota(jnp.int32, (channels, channels), 1)
    natural = lax.broadcasted_iota(jnp.int32, (channels, channels), 0)
    k, x = place % k_own, place // k_own % nx
    line = place // (k_own * nx)
    source = (x * nz + line) * k_own + k
    move = (natural == source).astype(BF16)
    source = (x * nz + line % nzh * nzl + line // nzh) * k_own + k
    move_one = (natural == source).astype(BF16)

    def moved(v, by):
        return jnp.dot(v, by, preferred_element_type=F32).astype(BF16)

    def own_half(v):
        return lax.dynamic_slice_in_dim(v, c * half, half, v.ndim - 1)

    core = c.astype(jnp.int32)[None]
    hold = pl.pallas_call(
        functools.partial(prep_kernel, nx, k_own),
        out_shape=jax.ShapeDtypeStruct((nx, 27, k_own, half), BF16),
        in_specs=[SM, VM, VM, VM],
        out_specs=VM,
        compiler_params=grant(60),
        name="prep",
    )(core, *[w.reshape(9, k_own, channels) for w in (first_weight, second_weight, upsample_weight)])
    hold = lax.all_to_all(hold, "x", 0, 0, tiled=True)
    hold = hold.transpose(1, 0, 2, 3).reshape(27, nx * k_own, half)
    weights = lax.all_gather(hold[9:], ("zh", "zl"))
    hold_one = hold[:9]

    own = features[0]
    wide = own.astype(F32)
    chan = lax.broadcasted_iota(jnp.int32, (channels, G), 0) // per_group
    member = (chan == lax.broadcasted_iota(jnp.int32, (channels, G), 1)).astype(F32)
    sums = jnp.stack([jnp.sum(wide, axis=0), jnp.sum(wide * wide, axis=0)])
    sums = jnp.dot(sums, member, precision=HIGHEST).reshape(1, 2 * G)
    sums = jnp.pad(sums, ((0, 0), (0, 128 - 2 * G)))
    sums = jnp.sum(sum_over(sums, ("x", "zl", "col")), axis=0, keepdims=True)
    high = lax.reduce_precision(sums, 8, 7)
    low = lax.reduce_precision(sums - high, 8, 7)
    terms = jnp.concatenate([high, low, sums - high - low]).astype(BF16)
    terms = jnp.pad(terms, ((0, nx * k_own - 3), (0, half - 128)))
    weights_one = lax.all_gather(jnp.concatenate([hold_one, terms[None]]), "zh")

    last = nx * nz - 1
    pairs = [(i, i + 1) for i in range(nzl - 1, last, nzl)] + [(i, i - 1) for i in range(nzl, last, nzl)]
    edge = lax.ppermute(own, ROW, pairs)
    sent = moved(jnp.concatenate([own, edge]), move_one)
    sent = sent.reshape(2, breadth, nzl, depth).transpose(2, 0, 1, 3)
    sent = jnp.broadcast_to(sent[:, None], (nzl, ncol, 2, breadth, depth))
    sent = sent.reshape(nzl * ncol, 2, breadth, depth)
    quad = lax.all_to_all(sent, ("zl", "col"), 0, 0, tiled=True)

    quad = quad.reshape(nzl, ncol, 2, breadth, depth)

    def own_depth(v):
        return lax.dynamic_slice_in_dim(v, zl * depth, depth, 1)

    gain_one = own_depth(order(first_gain, (2, 1, 0)))
    shift_one = own_depth(order(first_shift, (2, 1, 0)))
    vectors = order(jnp.stack([second_gain, second_shift, first_bias, second_bias]), (1, 2, 0))
    gain_two, shift_two = vectors[:1], vectors[1:2]
    vectors = own_half(jnp.concatenate([vectors[2:], upsample_bias[None]]))
    bias_one, bias_two, bias_up = [vectors[i : i + 1] for i in range(3)]

    def picks(group, groups):
        pick = group[:, None] == jnp.arange(128)[None, :]
        return jnp.concatenate([pick, jnp.roll(pick, groups, axis=1)]).astype(F32)

    lane = jnp.arange(depth)
    pick_one = picks(lane // k_own % nx * nzh + lane // (k_own * nx), G)
    lane = jnp.arange(channels)
    group = lane // (k_own * nx * nzl) * nx + lane // k_own % nx
    pick_two = picks(group, G)
    pick_own = picks(group[:half] + c * (G // ncol), G)

    parts = pl.pallas_call(
        functools.partial(conv_one_kernel, cols, image_rows, count),
        out_shape=jax.ShapeDtypeStruct((nzl, cols, half), BF16),
        in_specs=[SM] + [VM] * 5,
        out_specs=VM,
        scratch_shapes=[pltpu.VMEM(((nzl + 2) * cols, 3 * depth), BF16)],
        compiler_params=grant(16),
        name="conv_one",
    )(at, quad, gain_one, shift_one, pick_one, weights_one)
    parts, own = lax.optimization_barrier((parts, own))
    parts = lax.all_to_all(parts, "zl", 0, 0, tiled=True)
    three = [shifted_rows(own, ROW, -1), own, shifted_rows(own, ROW, 1)]
    hidden, sums_two = pl.pallas_call(
        join_kernel,
        out_shape=(
            jax.ShapeDtypeStruct((cols, half), BF16),
            jax.ShapeDtypeStruct((8, 128), F32),
        ),
        in_specs=[VM] * 3,
        out_specs=(VM, VM),
        compiler_params=grant(8),
        name="join_one",
    )(parts, bias_one, pick_own)

    both = lax.all_gather(hidden, "col")
    three, _ = lax.optimization_barrier((three, sums_two))
    stats = sum_over(sums_two[:1], ("x", "zl", "col"))
    stats = jnp.sum(stats, axis=0, keepdims=True)
    three = lax.all_gather(jnp.stack(three), "col", axis=1, tiled=True)
    residual = own_half(moved(three.reshape(3 * cols, channels), move))
    stats, both, residual = lax.optimization_barrier((stats, both, residual))
    stats = sum_over(stats, "zh")
    far = jnp.stack([lax.ppermute(both, ROW + ("col",), fetch(nx * nz, d)) for d in (1, 2)])
    far = lax.all_gather(far, "col")
    normed = pl.pallas_call(
        functools.partial(norm_kernel, image_rows, count),
        out_shape=jax.ShapeDtypeStruct((ncol, 5 * cols, half), BF16),
        in_specs=[SM] + [VM] * 6,
        out_specs=VM,
        compiler_params=grant(12),
        name="norm_two",
    )(at, both, far, stats, gain_two, shift_two, pick_two)

    rows = 3
    held = [
        pltpu.VMEM((2, nz // 2, 9) + weights.shape[2:], BF16),
        pltpu.SemaphoreType.DMA((2,)),
    ]
    block = pl.pallas_call(
        functools.partial(conv_two_kernel, cols, rows, image_rows),
        out_shape=jax.ShapeDtypeStruct((rows * cols, half), BF16),
        in_specs=[SM, VM, VM, VM, HB],
        out_specs=VM,
        scratch_shapes=held,
        compiler_params=grant(50),
        name="conv_two",
    )(at, normed, residual, bias_two, weights)
    block = lax.all_gather(block, "col")

    side = jax.ShapeDtypeStruct((2, cols, half), BF16)
    mine, theirs = pl.pallas_call(
        functools.partial(conv_up_kernel, cols),
        out_shape=(side, side),
        in_specs=[SM, VM, VM, VM],
        out_specs=(VM, VM),
        scratch_shapes=[pltpu.VMEM((2, 2, 2 * cols, 128), F32)],
        compiler_params=grant(16),
        name="conv_up",
    )(core, block, bias_up, weights)
    theirs = lax.ppermute(theirs, "col", [(0, 1), (1, 0)])
    return pl.pallas_call(
        sides_kernel,
        out_shape=jax.ShapeDtypeStruct((2, cols, channels), BF16),
        in_specs=[SM, VM, VM],
        out_specs=VM,
        compiler_params=grant(8),
        name="sides",
    )(core, mine, theirs)


def solution(mesh):
    finer = Mesh(
        mesh.devices.reshape(mesh.shape["img"], 4, 8, 4, mesh.shape["col"]),
        IMG_ROW + ("col",),
    )
    in_specs = (
        P(IMG_ROW, "col", None),
        P(),
        P(),
        P(None, None, ROW, None),
        P(),
        P(),
        P(),
        P(None, None, ROW, None),
        P(),
        P(None, None, ROW, None),
        P(),
    )

    return jax.shard_map(
        on_device,
        mesh=finer,
        in_specs=in_specs,
        out_specs=P(IMG_ROW, "col", None),
        check_vma=False,
    )
```

```python
import functools

import jax
import jax.numpy as jnp
from jax import lax
from jax.experimental import pallas as pl
from jax.experimental.pallas import tpu as pltpu
from jax.sharding import Mesh
from jax.sharding import PartitionSpec as P

G = 32
EPS = 1e-06
F32, BF16 = jnp.float32, jnp.bfloat16
HIGHEST = lax.Precision.HIGHEST
ROW = ("x", "zh", "zl")
IMG_ROW = ("img",) + ROW


def sum_over(vector, axes):
    count = lax.axis_size(axes)
    sent = jnp.broadcast_to(vector, (count, vector.shape[1]))
    return lax.all_to_all(sent, axes, 0, 0, tiled=True)


def shifted_rows(values, axis, by):
    count = lax.axis_size(axis)
    pairs = [(i, i - by) for i in range(count) if 0 <= i - by < count]
    return lax.ppermute(values, axis, pairs)


def fetch(count, by):
    above = [(2 * (i - by), 2 * i) for i in range(by, count)]
    return above + [(2 * (i + by) + 1, 2 * i + 1) for i in range(count - by)]


def silu(u):
    return u / (1.0 + jnp.exp(-u))


def spread_stats(totals, pick, count, gain, shift):
    totals = jnp.broadcast_to(totals, (8, totals.shape[1]))
    spread = lax.dot_general(
        totals, pick, (((1,), (1,)), ((), ())), precision=HIGHEST, preferred_element_type=F32
    )
    width = gain.shape[1]
    mean = spread[:1, :width] / count
    var = spread[:1, width:] / count - mean * mean
    a = lax.rsqrt(var + EPS) * gain
    return a, shift - mean * a


def conv_one_kernel(cols, image_rows, count, at_ref, x_ref, gain_ref, shift_ref, pick_ref, w_ref, out_ref, S):
    quad, depth = x_ref.shape[0], x_ref.shape[4]
    totals = jnp.sum(w_ref[:, 9, :, :128].astype(F32).reshape(-1, 128), axis=0, keepdims=True)
    a, b = spread_stats(totals, pick_ref[...], count, gain_ref[...], shift_ref[...])
    first = at_ref[0] // quad * quad - 1
    column = lax.broadcasted_iota(jnp.int32, (cols, depth), 0)
    for i in range(quad + 2):
        member = min(max(i - 1, 0), quad - 1)
        slot = 0 if 1 <= i <= quad else 1
        x = jnp.concatenate([x_ref[member, h, slot] for h in range(x_ref.shape[1])], axis=0)
        y = silu(x.astype(F32) * a + b)
        if slot:
            y = jnp.where(jnp.logical_and(first + i >= 0, first + i < image_rows), y, 0.0)
        at = slice(i * cols, (i + 1) * cols)
        left = jnp.where(column == 0, 0.0, pltpu.roll(y, 1, 0))
        right = jnp.where(column == cols - 1, 0.0, pltpu.roll(y, cols - 1, 0))
        S[at, 0 * depth : 1 * depth] = left.astype(BF16)
        S[at, 1 * depth : 2 * depth] = y.astype(BF16)
        S[at, 2 * depth : 3 * depth] = right.astype(BF16)
    outs = out_ref.shape[2]
    total = jnp.zeros((quad * cols, outs), F32)
    for r in range(3):
        piece = jnp.concatenate([w_ref[:, 3 * r + k].reshape(depth, outs) for k in range(3)], axis=0)
        total += jnp.dot(S[r * cols : (r + quad) * cols, :], piece, preferred_element_type=F32)
    out_ref[...] = total.astype(BF16).reshape(quad, cols, outs)


def join_kernel(x_ref, bias_ref, pick_ref, out_ref, sums_ref):
    total = x_ref[0].astype(F32)
    for k in range(1, x_ref.shape[0]):
        total += x_ref[k].astype(F32)
    hidden = (total + bias_ref[...]).astype(BF16)
    out_ref[...] = hidden
    own = hidden.astype(F32)
    both = jnp.concatenate(
        [jnp.sum(own, axis=0, keepdims=True), jnp.sum(own * own, axis=0, keepdims=True)], axis=1
    )
    both = jnp.broadcast_to(both, (8, both.shape[1]))
    sums_ref[...] = jnp.dot(both, pick_ref[...], precision=HIGHEST, preferred_element_type=F32)


def norm_kernel(image_rows, count, at_ref, own_ref, far_ref, stats_ref, gain_ref, shift_ref, pick_ref, out_ref):
    totals = jnp.sum(stats_ref[...], axis=0, keepdims=True)
    a, b = spread_stats(totals, pick_ref[...], count, gain_ref[...], shift_ref[...])
    halves, cols, half = own_ref.shape
    for d in range(-2, 3):
        row = at_ref[0] + d
        inside = jnp.logical_and(row >= 0, row < image_rows)
        for h in range(halves):
            lanes = slice(h * half, (h + 1) * half)
            x = far_ref[int(d > 0), abs(d) - 1, h] if d else own_ref[h]
            y = silu(x.astype(F32) * a[:, lanes] + b[:, lanes])
            out_ref[h, (d + 2) * cols : (d + 3) * cols, :] = jnp.where(inside, y, 0.0).astype(BF16)


def fetch_weights(w_ref, held, arrived):
    lines = held.shape[2]
    copies = [
        [
            pltpu.make_async_copy(
                w_ref.at[pl.ds(h * lines, lines), pl.ds(3 * r, 3)], held.at[h, r], arrived.at[h, r]
            )
            for r in range(3)
        ]
        for h in range(2)
    ]
    for half in copies:
        for copy in half:
            copy.start()
    return copies


def moved_right(y, cols):
    column = lax.broadcasted_iota(jnp.int32, y.shape, 0) % cols
    return jnp.where(column == 0, 0.0, pltpu.roll(y, 1, 0))


def moved_left(y, cols):
    column = lax.broadcasted_iota(jnp.int32, y.shape, 0) % cols
    return jnp.where(column == cols - 1, 0.0, pltpu.roll(y, y.shape[0] - 1, 0))


def conv_two_kernel(cols, rows, image_rows, at_ref, x_ref, res_ref, bias_ref, w_ref, out_ref, held, arrived):
    copies = fetch_weights(w_ref, held, arrived)
    outs = out_ref.shape[1]
    totals = [jnp.zeros(out_ref.shape, F32) for _ in range(3)]
    for h in range(2):
        for r in range(3):
            copies[h][r].wait()
            x = x_ref[h, r * cols : (r + rows) * cols, :]
            for k in range(3):
                piece = held[h, r, :, k].reshape(-1, outs)
                totals[k] += jnp.dot(x, piece, preferred_element_type=F32)
    total = totals[1] + moved_right(totals[0], cols) + moved_left(totals[2], cols) + bias_ref[...]
    first = at_ref[0] - rows // 2
    for i in range(rows):
        at = slice(i * cols, (i + 1) * cols)
        y = total[at] + res_ref[at, :].astype(F32)
        inside = jnp.logical_and(first + i >= 0, first + i < image_rows)
        out_ref[at, :] = jnp.where(inside, y, 0.0).astype(BF16)


def conv_up_kernel(cols, at_ref, x_ref, bias_ref, w_ref, mine_ref, theirs_ref, full):
    lines = w_ref.shape[0] // 2
    outs = mine_ref.shape[2]
    totals = [jnp.zeros((2 * cols, outs), F32) for _ in range(3)]
    for h in range(2):
        for r in range(3):
            starts = [(r + 1 + p) // 2 * cols for p in range(2)]
            x = jnp.concatenate([x_ref[h, start : start + cols, :] for start in starts])
            for k in range(3):
                piece = w_ref[h * lines : (h + 1) * lines, 9 + 3 * r + k].reshape(-1, outs)
                totals[k] += jnp.dot(x, piece, preferred_element_type=F32)
    middle = totals[1] + bias_ref[...]
    even = moved_right(totals[0], cols) + middle + totals[2]
    odd = totals[0] + middle + moved_left(totals[2], cols)
    mine = pl.multiple_of(at_ref[0] * cols, cols)
    theirs = pl.multiple_of((1 - at_ref[0]) * cols, cols)
    for p in range(2):
        for k in range(2):
            lanes = slice(k * 128, (k + 1) * 128)
            for q, y in enumerate((even, odd)):
                full[p, k, pl.ds(q, cols, stride=2), :] = y[p * cols : (p + 1) * cols, lanes]
            mine_ref[p, :, lanes] = full[p, k, pl.ds(mine, cols), :].astype(BF16)
            theirs_ref[p, :, lanes] = full[p, k, pl.ds(theirs, cols), :].astype(BF16)


def sides_kernel(at_ref, mine_ref, theirs_ref, out_ref):
    outs = mine_ref.shape[2]
    for k, first, second in ((0, mine_ref, theirs_ref), (1, theirs_ref, mine_ref)):

        @pl.when(at_ref[0] == k)
        def _():
            out_ref[:, :, :outs] = first[...]
            out_ref[:, :, outs:] = second[...]


def grant(mebibytes):
    return pltpu.CompilerParams(vmem_limit_bytes=mebibytes << 20)


VM = pl.BlockSpec(memory_space=pltpu.VMEM)
SM = pl.BlockSpec(memory_space=pltpu.SMEM)
HB = pl.BlockSpec(memory_space=pltpu.HBM)


def on_device(
    features,
    first_gain,
    first_shift,
    first_weight,
    first_bias,
    second_gain,
    second_shift,
    second_weight,
    second_bias,
    upsample_weight,
    upsample_bias,
):
    _, breadth, channels = features.shape
    nx, nzh, nzl, ncol = (lax.axis_size(axis) for axis in ("x", "zh", "zl", "col"))
    nz = nzh * nzl
    k_own = first_weight.shape[2]
    cols = breadth * ncol
    half = channels // ncol
    depth = channels // nzl
    image_rows = nx * nz
    per_group = channels // G
    count = image_rows * cols * per_group
    c = lax.axis_index("col")
    zl = lax.axis_index("zl")
    at = lax.axis_index(ROW).astype(jnp.int32)[None]

    def order(v, axes):
        v = v.reshape(-1, nx, nzh, nzl, k_own).transpose(0, *[k + 1 for k in axes], 4)
        return v.reshape(-1, channels)

    place = lax.broadcasted_iota(jnp.int32, (channels, channels), 1)
    natural = lax.broadcasted_iota(jnp.int32, (channels, channels), 0)
    k, x = place % k_own, place // k_own % nx
    line = place // (k_own * nx)
    source = (x * nz + line) * k_own + k
    move = (natural == source).astype(BF16)
    source = (x * nz + line % nzh * nzl + line // nzh) * k_own + k
    move_one = (natural == source).astype(BF16)

    def moved(v, by):
        return jnp.dot(v, by, preferred_element_type=F32).astype(BF16)

    def own_half(v):
        return lax.dynamic_slice_in_dim(v, c * half, half, v.ndim - 1)

    taps = 9 * k_own
    hold = moved(
        jnp.concatenate([first_weight.reshape(taps, channels), second_weight.reshape(taps, channels)]),
        move,
    )
    hold = jnp.concatenate([hold, upsample_weight.reshape(taps, channels)])
    hold = own_half(hold).reshape(1, 27, k_own, half)
    hold = lax.all_to_all(jnp.broadcast_to(hold, (nx, 27, k_own, half)), "x", 0, 0, tiled=True)
    hold = hold.transpose(1, 0, 2, 3).reshape(27, nx * k_own, half)
    weights = lax.all_gather(hold[9:], ("zh", "zl"))
    hold_one = hold[:9]

    own = features[0]
    wide = own.astype(F32)
    chan = lax.broadcasted_iota(jnp.int32, (channels, G), 0) // per_group
    member = (chan == lax.broadcasted_iota(jnp.int32, (channels, G), 1)).astype(F32)
    sums = jnp.stack([jnp.sum(wide, axis=0), jnp.sum(wide * wide, axis=0)])
    sums = jnp.dot(sums, member, precision=HIGHEST).reshape(1, 2 * G)
    sums = jnp.pad(sums, ((0, 0), (0, 128 - 2 * G)))
    sums = jnp.sum(sum_over(sums, ("x", "zl", "col")), axis=0, keepdims=True)
    high = lax.reduce_precision(sums, 8, 7)
    low = lax.reduce_precision(sums - high, 8, 7)
    terms = jnp.concatenate([high, low, sums - high - low]).astype(BF16)
    terms = jnp.pad(terms, ((0, nx * k_own - 3), (0, half - 128)))
    weights_one = lax.all_gather(jnp.concatenate([hold_one, terms[None]]), "zh")

    last = nx * nz - 1
    pairs = [(i, i + 1) for i in range(nzl - 1, last, nzl)] + [(i, i - 1) for i in range(nzl, last, nzl)]
    edge = lax.ppermute(own, ROW, pairs)
    sent = moved(jnp.concatenate([own, edge]), move_one)
    sent = sent.reshape(2, breadth, nzl, depth).transpose(2, 0, 1, 3)
    sent = jnp.broadcast_to(sent[:, None], (nzl, ncol, 2, breadth, depth))
    sent = sent.reshape(nzl * ncol, 2, breadth, depth)
    quad = lax.all_to_all(sent, ("zl", "col"), 0, 0, tiled=True)

    quad = quad.reshape(nzl, ncol, 2, breadth, depth)

    def own_depth(v):
        return lax.dynamic_slice_in_dim(v, zl * depth, depth, 1)

    gain_one = own_depth(order(first_gain, (2, 1, 0)))
    shift_one = own_depth(order(first_shift, (2, 1, 0)))
    vectors = order(jnp.stack([second_gain, second_shift, first_bias, second_bias]), (1, 2, 0))
    gain_two, shift_two = vectors[:1], vectors[1:2]
    vectors = own_half(jnp.concatenate([vectors[2:], upsample_bias[None]]))
    bias_one, bias_two, bias_up = [vectors[i : i + 1] for i in range(3)]

    def picks(group, groups):
        pick = group[:, None] == jnp.arange(128)[None, :]
        return jnp.concatenate([pick, jnp.roll(pick, groups, axis=1)]).astype(F32)

    lane = jnp.arange(depth)
    pick_one = picks(lane // k_own % nx * nzh + lane // (k_own * nx), G)
    lane = jnp.arange(channels)
    group = lane // (k_own * nx * nzl) * nx + lane // k_own % nx
    pick_two = picks(group, G)
    pick_own = picks(group[:half] + c * (G // ncol), G)

    parts = pl.pallas_call(
        functools.partial(conv_one_kernel, cols, image_rows, count),
        out_shape=jax.ShapeDtypeStruct((nzl, cols, half), BF16),
        in_specs=[SM] + [VM] * 5,
        out_specs=VM,
        scratch_shapes=[pltpu.VMEM(((nzl + 2) * cols, 3 * depth), BF16)],
        compiler_params=grant(16),
        name="conv_one",
    )(at, quad, gain_one, shift_one, pick_one, weights_one)
    parts, own = lax.optimization_barrier((parts, own))
    parts = lax.all_to_all(parts, "zl", 0, 0, tiled=True)
    three = [shifted_rows(own, ROW, -1), own, shifted_rows(own, ROW, 1)]
    hidden, sums_two = pl.pallas_call(
        join_kernel,
        out_shape=(
            jax.ShapeDtypeStruct((cols, half), BF16),
            jax.ShapeDtypeStruct((8, 128), F32),
        ),
        in_specs=[VM] * 3,
        out_specs=(VM, VM),
        compiler_params=grant(8),
        name="join_one",
    )(parts, bias_one, pick_own)

    both = lax.all_gather(hidden, "col")
    three, _ = lax.optimization_barrier((three, sums_two))
    stats = sum_over(sums_two[:1], ("x", "zl", "col"))
    stats = jnp.sum(stats, axis=0, keepdims=True)
    three = lax.all_gather(jnp.stack(three), "col", axis=1, tiled=True)
    residual = own_half(moved(three.reshape(3 * cols, channels), move))
    stats, both, residual = lax.optimization_barrier((stats, both, residual))
    stats = sum_over(stats, "zh")
    far = jnp.stack([lax.ppermute(both, ROW + ("col",), fetch(nx * nz, d)) for d in (1, 2)])
    far = lax.all_gather(far, "col")
    normed = pl.pallas_call(
        functools.partial(norm_kernel, image_rows, count),
        out_shape=jax.ShapeDtypeStruct((ncol, 5 * cols, half), BF16),
        in_specs=[SM] + [VM] * 6,
        out_specs=VM,
        compiler_params=grant(12),
        name="norm_two",
    )(at, both, far, stats, gain_two, shift_two, pick_two)

    rows = 3
    held = [
        pltpu.VMEM((2, 3, nz // 2, 3) + weights.shape[2:], BF16),
        pltpu.SemaphoreType.DMA((2, 3)),
    ]
    block = pl.pallas_call(
        functools.partial(conv_two_kernel, cols, rows, image_rows),
        out_shape=jax.ShapeDtypeStruct((rows * cols, half), BF16),
        in_specs=[SM, VM, VM, VM, HB],
        out_specs=VM,
        scratch_shapes=held,
        compiler_params=grant(50),
        name="conv_two",
    )(at, normed, residual, bias_two, weights)
    block = lax.all_gather(block, "col")

    core = c.astype(jnp.int32)[None]
    side = jax.ShapeDtypeStruct((2, cols, half), BF16)
    mine, theirs = pl.pallas_call(
        functools.partial(conv_up_kernel, cols),
        out_shape=(side, side),
        in_specs=[SM, VM, VM, VM],
        out_specs=(VM, VM),
        scratch_shapes=[pltpu.VMEM((2, 2, 2 * cols, 128), F32)],
        compiler_params=grant(16),
        name="conv_up",
    )(core, block, bias_up, weights)
    theirs = lax.ppermute(theirs, "col", [(0, 1), (1, 0)])
    return pl.pallas_call(
        sides_kernel,
        out_shape=jax.ShapeDtypeStruct((2, cols, channels), BF16),
        in_specs=[SM, VM, VM],
        out_specs=VM,
        compiler_params=grant(8),
        name="sides",
    )(core, mine, theirs)


def solution(mesh):
    finer = Mesh(
        mesh.devices.reshape(mesh.shape["img"], 4, 8, 4, mesh.shape["col"]),
        IMG_ROW + ("col",),
    )
    in_specs = (
        P(IMG_ROW, "col", None),
        P(),
        P(),
        P(None, None, ROW, None),
        P(),
        P(),
        P(),
        P(None, None, ROW, None),
        P(),
        P(None, None, ROW, None),
        P(),
    )

    return jax.shard_map(
        on_device,
        mesh=finer,
        in_specs=in_specs,
        out_specs=P(IMG_ROW, "col", None),
        check_vma=False,
    )
```

```python
import functools

import jax
import jax.numpy as jnp
from jax import lax
from jax.experimental import pallas as pl
from jax.experimental.pallas import tpu as pltpu
from jax.sharding import Mesh
from jax.sharding import PartitionSpec as P

G = 32
EPS = 1e-06
F32, BF16 = jnp.float32, jnp.bfloat16
HIGHEST = lax.Precision.HIGHEST
ROW = ("x", "zh", "zl")
IMG_ROW = ("img",) + ROW


def sum_over(vector, axes):
    count = lax.axis_size(axes)
    sent = jnp.broadcast_to(vector, (count, vector.shape[1]))
    return lax.all_to_all(sent, axes, 0, 0, tiled=True)


def shifted_rows(values, axis, by):
    count = lax.axis_size(axis)
    pairs = [(i, i - by) for i in range(count) if 0 <= i - by < count]
    return lax.ppermute(values, axis, pairs)


def fetch(count, by):
    above = [(2 * (i - by), 2 * i) for i in range(by, count)]
    return above + [(2 * (i + by) + 1, 2 * i + 1) for i in range(count - by)]


def silu(u):
    return u / (1.0 + jnp.exp(-u))


def prep_kernel(nx, core_ref, w_ref, out_ref):
    taps, k_own, channels = w_ref.shape
    moving, half = taps // 3 * 2, out_ref.shape[3]
    place = lax.broadcasted_iota(jnp.int32, (channels, half), 1) + core_ref[0] * half
    natural = lax.broadcasted_iota(jnp.int32, (channels, half), 0)
    line, x, k = place // (k_own * nx), place // k_own % nx, place % k_own
    move = (natural == (x * (channels // (nx * k_own)) + line) * k_own + k).astype(BF16)
    rows = jnp.concatenate([w_ref[t].astype(F32) for t in range(moving)]).astype(BF16)
    moved = jnp.dot(rows, move, preferred_element_type=F32)
    lanes = pl.ds(pl.multiple_of(core_ref[0] * half, half), half)
    for d in range(nx):
        for t in range(moving):
            out_ref[d, t] = moved[t * k_own : (t + 1) * k_own].astype(BF16)
        out_ref[d, moving:] = w_ref[moving:, :, lanes]


def spread_stats(totals, pick, count, gain, shift):
    totals = jnp.broadcast_to(totals, (8, totals.shape[1]))
    spread = lax.dot_general(
        totals, pick, (((1,), (1,)), ((), ())), precision=HIGHEST, preferred_element_type=F32
    )
    width = gain.shape[1]
    mean = spread[:1, :width] / count
    var = spread[:1, width:] / count - mean * mean
    a = lax.rsqrt(var + EPS) * gain
    return a, shift - mean * a


def conv_one_kernel(cols, image_rows, count, at_ref, x_ref, gain_ref, shift_ref, pick_ref, w_ref, out_ref, S):
    quad, depth = x_ref.shape[0], x_ref.shape[4]
    totals = jnp.sum(w_ref[:, 9, :, :128].astype(F32).reshape(-1, 128), axis=0, keepdims=True)
    a, b = spread_stats(totals, pick_ref[...], count, gain_ref[...], shift_ref[...])
    first = at_ref[0] // quad * quad - 1
    column = lax.broadcasted_iota(jnp.int32, (cols, depth), 0)
    for i in range(quad + 2):
        member = min(max(i - 1, 0), quad - 1)
        slot = 0 if 1 <= i <= quad else 1
        x = jnp.concatenate([x_ref[member, h, slot] for h in range(x_ref.shape[1])], axis=0)
        y = silu(x.astype(F32) * a + b)
        if slot:
            y = jnp.where(jnp.logical_and(first + i >= 0, first + i < image_rows), y, 0.0)
        at = slice(i * cols, (i + 1) * cols)
        left = jnp.where(column == 0, 0.0, pltpu.roll(y, 1, 0))
        right = jnp.where(column == cols - 1, 0.0, pltpu.roll(y, cols - 1, 0))
        S[at, 0 * depth : 1 * depth] = left.astype(BF16)
        S[at, 1 * depth : 2 * depth] = y.astype(BF16)
        S[at, 2 * depth : 3 * depth] = right.astype(BF16)
    outs = out_ref.shape[2]
    total = jnp.zeros((quad * cols, outs), F32)
    for r in range(3):
        piece = jnp.concatenate([w_ref[:, 3 * r + k].reshape(depth, outs) for k in range(3)], axis=0)
        total += jnp.dot(S[r * cols : (r + quad) * cols, :], piece, preferred_element_type=F32)
    out_ref[...] = total.astype(BF16).reshape(quad, cols, outs)


def join_kernel(x_ref, bias_ref, pick_ref, out_ref, sums_ref):
    total = x_ref[0].astype(F32)
    for k in range(1, x_ref.shape[0]):
        total += x_ref[k].astype(F32)
    hidden = (total + bias_ref[...]).astype(BF16)
    out_ref[...] = hidden
    own = hidden.astype(F32)
    both = jnp.concatenate(
        [jnp.sum(own, axis=0, keepdims=True), jnp.sum(own * own, axis=0, keepdims=True)], axis=1
    )
    both = jnp.broadcast_to(both, (8, both.shape[1]))
    sums_ref[...] = jnp.dot(both, pick_ref[...], precision=HIGHEST, preferred_element_type=F32)


def norm_kernel(image_rows, count, at_ref, own_ref, far_ref, stats_ref, gain_ref, shift_ref, pick_ref, out_ref):
    totals = jnp.sum(stats_ref[...], axis=0, keepdims=True)
    a, b = spread_stats(totals, pick_ref[...], count, gain_ref[...], shift_ref[...])
    halves, cols, half = own_ref.shape
    for d in range(-2, 3):
        row = at_ref[0] + d
        inside = jnp.logical_and(row >= 0, row < image_rows)
        for h in range(halves):
            lanes = slice(h * half, (h + 1) * half)
            x = far_ref[int(d > 0), abs(d) - 1, h] if d else own_ref[h]
            y = silu(x.astype(F32) * a[:, lanes] + b[:, lanes])
            out_ref[h, (d + 2) * cols : (d + 3) * cols, :] = jnp.where(inside, y, 0.0).astype(BF16)


def fetch_weights(w_ref, held, arrived):
    lines = held.shape[1]
    copies = [
        pltpu.make_async_copy(
            w_ref.at[pl.ds(h * lines, lines), pl.ds(0, 9)], held.at[h], arrived.at[h]
        )
        for h in range(2)
    ]
    for copy in copies:
        copy.start()
    return copies


def moved_right(y, cols):
    column = lax.broadcasted_iota(jnp.int32, y.shape, 0) % cols
    return jnp.where(column == 0, 0.0, pltpu.roll(y, 1, 0))


def moved_left(y, cols):
    column = lax.broadcasted_iota(jnp.int32, y.shape, 0) % cols
    return jnp.where(column == cols - 1, 0.0, pltpu.roll(y, y.shape[0] - 1, 0))


def conv_two_kernel(cols, rows, image_rows, at_ref, x_ref, res_ref, bias_ref, w_ref, out_ref, held, arrived):
    copies = fetch_weights(w_ref, held, arrived)
    outs = out_ref.shape[1]
    totals = [jnp.zeros(out_ref.shape, F32) for _ in range(3)]
    for h in range(2):
        copies[h].wait()
        for r in range(3):
            x = x_ref[h, r * cols : (r + rows) * cols, :]
            for k in range(3):
                piece = held[h, :, 3 * r + k].reshape(-1, outs)
                totals[k] += jnp.dot(x, piece, preferred_element_type=F32)
    total = totals[1] + moved_right(totals[0], cols) + moved_left(totals[2], cols) + bias_ref[...]
    first = at_ref[0] - rows // 2
    for i in range(rows):
        at = slice(i * cols, (i + 1) * cols)
        y = total[at] + res_ref[at, :].astype(F32)
        inside = jnp.logical_and(first + i >= 0, first + i < image_rows)
        out_ref[at, :] = jnp.where(inside, y, 0.0).astype(BF16)


def conv_up_kernel(cols, at_ref, x_ref, bias_ref, w_ref, mine_ref, theirs_ref, full):
    lines = w_ref.shape[0] // 2
    outs = mine_ref.shape[2]
    totals = [jnp.zeros((2 * cols, outs), F32) for _ in range(3)]
    for h in range(2):
        for r in range(3):
            starts = [(r + 1 + p) // 2 * cols for p in range(2)]
            x = jnp.concatenate([x_ref[h, start : start + cols, :] for start in starts])
            for k in range(3):
                piece = w_ref[h * lines : (h + 1) * lines, 9 + 3 * r + k].reshape(-1, outs)
                totals[k] += jnp.dot(x, piece, preferred_element_type=F32)
    middle = totals[1] + bias_ref[...]
    even = moved_right(totals[0], cols) + middle + totals[2]
    odd = totals[0] + middle + moved_left(totals[2], cols)
    mine = pl.multiple_of(at_ref[0] * cols, cols)
    theirs = pl.multiple_of((1 - at_ref[0]) * cols, cols)
    for p in range(2):
        for k in range(2):
            lanes = slice(k * 128, (k + 1) * 128)
            for q, y in enumerate((even, odd)):
                full[p, k, pl.ds(q, cols, stride=2), :] = y[p * cols : (p + 1) * cols, lanes]
            mine_ref[p, :, lanes] = full[p, k, pl.ds(mine, cols), :].astype(BF16)
            theirs_ref[p, :, lanes] = full[p, k, pl.ds(theirs, cols), :].astype(BF16)


def sides_kernel(at_ref, mine_ref, theirs_ref, out_ref):
    outs = mine_ref.shape[2]
    for k, first, second in ((0, mine_ref, theirs_ref), (1, theirs_ref, mine_ref)):

        @pl.when(at_ref[0] == k)
        def _():
            out_ref[:, :, :outs] = first[...]
            out_ref[:, :, outs:] = second[...]


def grant(mebibytes):
    return pltpu.CompilerParams(vmem_limit_bytes=mebibytes << 20)


VM = pl.BlockSpec(memory_space=pltpu.VMEM)
SM = pl.BlockSpec(memory_space=pltpu.SMEM)
HB = pl.BlockSpec(memory_space=pltpu.HBM)


def on_device(
    features,
    first_gain,
    first_shift,
    first_weight,
    first_bias,
    second_gain,
    second_shift,
    second_weight,
    second_bias,
    upsample_weight,
    upsample_bias,
):
    _, breadth, channels = features.shape
    nx, nzh, nzl, ncol = (lax.axis_size(axis) for axis in ("x", "zh", "zl", "col"))
    nz = nzh * nzl
    k_own = first_weight.shape[2]
    cols = breadth * ncol
    half = channels // ncol
    depth = channels // nzl
    image_rows = nx * nz
    per_group = channels // G
    count = image_rows * cols * per_group
    c = lax.axis_index("col")
    zl = lax.axis_index("zl")
    at = lax.axis_index(ROW).astype(jnp.int32)[None]

    def order(v, axes):
        v = v.reshape(-1, nx, nzh, nzl, k_own).transpose(0, *[k + 1 for k in axes], 4)
        return v.reshape(-1, channels)

    place = lax.broadcasted_iota(jnp.int32, (channels, channels), 1)
    natural = lax.broadcasted_iota(jnp.int32, (channels, channels), 0)
    k, x = place % k_own, place // k_own % nx
    line = place // (k_own * nx)
    source = (x * nz + line) * k_own + k
    move = (natural == source).astype(BF16)
    source = (x * nz + line % nzh * nzl + line // nzh) * k_own + k
    move_one = (natural == source).astype(BF16)

    def moved(v, by):
        return jnp.dot(v, by, preferred_element_type=F32).astype(BF16)

    def own_half(v):
        return lax.dynamic_slice_in_dim(v, c * half, half, v.ndim - 1)

    core = c.astype(jnp.int32)[None]
    hold = [w.reshape(9, k_own, channels) for w in (first_weight, second_weight, upsample_weight)]
    hold = pl.pallas_call(
        functools.partial(prep_kernel, nx),
        out_shape=jax.ShapeDtypeStruct((nx, 27, k_own, half), BF16),
        in_specs=[SM, VM],
        out_specs=VM,
        compiler_params=grant(16),
        name="prep",
    )(core, jnp.concatenate(hold))
    hold = lax.all_to_all(hold, "x", 0, 0, tiled=True)
    hold = hold.transpose(1, 0, 2, 3).reshape(27, nx * k_own, half)
    weights = lax.all_gather(hold[9:], ("zh", "zl"))
    hold_one = hold[:9]

    own = features[0]
    wide = own.astype(F32)
    chan = lax.broadcasted_iota(jnp.int32, (channels, G), 0) // per_group
    member = (chan == lax.broadcasted_iota(jnp.int32, (channels, G), 1)).astype(F32)
    sums = jnp.stack([jnp.sum(wide, axis=0), jnp.sum(wide * wide, axis=0)])
    sums = jnp.dot(sums, member, precision=HIGHEST).reshape(1, 2 * G)
    sums = jnp.pad(sums, ((0, 0), (0, 128 - 2 * G)))
    sums = sum_over(sums, ("x", "zl", "col"))
    sums = jnp.sum(sums, axis=0, keepdims=True)
    high = lax.reduce_precision(sums, 8, 7)
    low = lax.reduce_precision(sums - high, 8, 7)
    terms = jnp.concatenate([high, low, sums - high - low]).astype(BF16)
    terms = jnp.pad(terms, ((0, nx * k_own - 3), (0, half - 128)))
    weights_one = lax.all_gather(jnp.concatenate([hold_one, terms[None]]), "zh")

    last = nx * nz - 1
    pairs = [(i, i + 1) for i in range(nzl - 1, last, nzl)] + [(i, i - 1) for i in range(nzl, last, nzl)]
    edge = lax.ppermute(own, ROW, pairs)
    sent = moved(jnp.concatenate([own, edge]), move_one)
    sent = sent.reshape(2, breadth, nzl, depth).transpose(2, 0, 1, 3)
    sent = jnp.broadcast_to(sent[:, None], (nzl, ncol, 2, breadth, depth))
    sent = sent.reshape(nzl * ncol, 2, breadth, depth)
    quad = lax.all_to_all(sent, ("zl", "col"), 0, 0, tiled=True)

    quad = quad.reshape(nzl, ncol, 2, breadth, depth)

    def own_depth(v):
        return lax.dynamic_slice_in_dim(v, zl * depth, depth, 1)

    gain_one = own_depth(order(first_gain, (2, 1, 0)))
    shift_one = own_depth(order(first_shift, (2, 1, 0)))
    vectors = order(jnp.stack([second_gain, second_shift, first_bias, second_bias]), (1, 2, 0))
    gain_two, shift_two = vectors[:1], vectors[1:2]
    vectors = own_half(jnp.concatenate([vectors[2:], upsample_bias[None]]))
    bias_one, bias_two, bias_up = [vectors[i : i + 1] for i in range(3)]

    def picks(group, groups):
        pick = group[:, None] == jnp.arange(128)[None, :]
        return jnp.concatenate([pick, jnp.roll(pick, groups, axis=1)]).astype(F32)

    lane = jnp.arange(depth)
    pick_one = picks(lane // k_own % nx * nzh + lane // (k_own * nx), G)
    lane = jnp.arange(channels)
    group = lane // (k_own * nx * nzl) * nx + lane // k_own % nx
    pick_two = picks(group, G)
    pick_own = picks(group[:half] + c * (G // ncol), G)

    parts = pl.pallas_call(
        functools.partial(conv_one_kernel, cols, image_rows, count),
        out_shape=jax.ShapeDtypeStruct((nzl, cols, half), BF16),
        in_specs=[SM] + [VM] * 5,
        out_specs=VM,
        scratch_shapes=[pltpu.VMEM(((nzl + 2) * cols, 3 * depth), BF16)],
        compiler_params=grant(16),
        name="conv_one",
    )(at, quad, gain_one, shift_one, pick_one, weights_one)
    parts, own = lax.optimization_barrier((parts, own))
    parts = lax.all_to_all(parts, "zl", 0, 0, tiled=True)
    three = [shifted_rows(own, ROW, -1), own, shifted_rows(own, ROW, 1)]
    hidden, sums_two = pl.pallas_call(
        join_kernel,
        out_shape=(
            jax.ShapeDtypeStruct((cols, half), BF16),
            jax.ShapeDtypeStruct((8, 128), F32),
        ),
        in_specs=[VM] * 3,
        out_specs=(VM, VM),
        compiler_params=grant(8),
        name="join_one",
    )(parts, bias_one, pick_own)

    both = lax.all_gather(hidden, "col")
    three, _ = lax.optimization_barrier((three, sums_two))
    stats = sum_over(sums_two[:1], ("x", "zl", "col"))
    stats = jnp.sum(stats, axis=0, keepdims=True)
    three = lax.all_gather(jnp.stack(three), "col", axis=1, tiled=True)
    residual = own_half(moved(three.reshape(3 * cols, channels), move))
    stats, both = lax.optimization_barrier((stats, both))
    stats = sum_over(stats, "zh")
    far = jnp.stack([lax.ppermute(both, ROW + ("col",), fetch(nx * nz, d)) for d in (1, 2)])
    far = lax.all_gather(far, "col")
    normed = pl.pallas_call(
        functools.partial(norm_kernel, image_rows, count),
        out_shape=jax.ShapeDtypeStruct((ncol, 5 * cols, half), BF16),
        in_specs=[SM] + [VM] * 6,
        out_specs=VM,
        compiler_params=grant(12),
        name="norm_two",
    )(at, both, far, stats, gain_two, shift_two, pick_two)

    rows = 3
    held = [
        pltpu.VMEM((2, nz // 2, 9) + weights.shape[2:], BF16),
        pltpu.SemaphoreType.DMA((2,)),
    ]
    block = pl.pallas_call(
        functools.partial(conv_two_kernel, cols, rows, image_rows),
        out_shape=jax.ShapeDtypeStruct((rows * cols, half), BF16),
        in_specs=[SM, VM, VM, VM, HB],
        out_specs=VM,
        scratch_shapes=held,
        compiler_params=grant(50),
        name="conv_two",
    )(at, normed, residual, bias_two, weights)
    block = lax.all_gather(block, "col")

    side = jax.ShapeDtypeStruct((2, cols, half), BF16)
    mine, theirs = pl.pallas_call(
        functools.partial(conv_up_kernel, cols),
        out_shape=(side, side),
        in_specs=[SM, VM, VM, VM],
        out_specs=(VM, VM),
        scratch_shapes=[pltpu.VMEM((2, 2, 2 * cols, 128), F32)],
        compiler_params=grant(16),
        name="conv_up",
    )(core, block, bias_up, weights)
    theirs = lax.ppermute(theirs, "col", [(0, 1), (1, 0)])
    return pl.pallas_call(
        sides_kernel,
        out_shape=jax.ShapeDtypeStruct((2, cols, channels), BF16),
        in_specs=[SM, VM, VM],
        out_specs=VM,
        compiler_params=grant(8),
        name="sides",
    )(core, mine, theirs)


def solution(mesh):
    finer = Mesh(
        mesh.devices.reshape(mesh.shape["img"], 4, 8, 4, mesh.shape["col"]),
        IMG_ROW + ("col",),
    )
    in_specs = (
        P(IMG_ROW, "col", None),
        P(),
        P(),
        P(None, None, ROW, None),
        P(),
        P(),
        P(),
        P(None, None, ROW, None),
        P(),
        P(None, None, ROW, None),
        P(),
    )

    return jax.shard_map(
        on_device,
        mesh=finer,
        in_specs=in_specs,
        out_specs=P(IMG_ROW, "col", None),
        check_vma=False,
    )
```
